128 devices in a mesh: row: 16 (over x, z), col: 8 (over y, core).
Axes of the slice: x: 4, y: 4, z: 4, core: 2. Of those that a mesh axis runs over, the one named last changes fastest.
Arguments:
- basis_blocks: float32 [8, 16, 1048576], P(None, None, ('col', 'row')), may hold values from -6 to 6
- tile_values: bfloat16 [8, 16, 384, 128, 128], P('col', 'row'), may hold values from -0.375 to 0.375
- tile_rows: int32 [8, 16, 384], P('col', 'row'), may hold values from 0 to 1023
- tile_column: int32 [8, 16, 384], P('col', 'row'), may hold values from 0 to 511
- tile_count: int32 [8, 16], P('col', 'row'), may hold values from 1 to 384, as said below
- diagonal: float32 [1048576], P(('col', 'row')), may hold values from 1 to 6
Outputs:
- new_block: float32 [16, 1048576], P(None, ('col', 'row'))
- coefficients: float32 [8, 16, 16], replicated
- triangle: float32 [16, 16], replicated
The draws below stay inside these ranges and needn't reach their ends.
Inputs may be any that keep to these rules, and one draw needn't show every extreme that they name: Each operator block stores tile_count tiles in its first slots; at most 384, and some block has exactly 384 in every draw. Slots past the count hold arbitrary data and are ignored.
All inputs are finite; a program needn't handle non-finite values.
Results may differ from the reference program's by a relative error of at most 0.0031.
Values may be sent and summed in bfloat16 or wider, within the bound.
A program may use at most 128 MiB of HBM per device.

```python
import math
import jax
import jax.numpy as jnp
import numpy as np
from jax import lax

RHS = 16
BLOCKS = 8
TILE = 128
TMAX = 384
ORDER = 1048576
BLOCK_ROWS = 131072
BLOCK_COLS = 65536
N_ROW = 16
N_COL = 8


def draw_basis_blocks(key, part):
    return jnp.clip(jax.random.normal(key, (BLOCKS, RHS, ORDER), jnp.float32), -6.0, 6.0)


def draw_tile_count(key, part):
    divisor = 1 + jax.random.randint(key, (N_COL, N_ROW), 0, 8)
    base_count = jnp.maximum(TMAX // divisor, 1)
    hub_index = jax.random.randint(jax.random.fold_in(key, 3), (), 0, N_COL * N_ROW)
    flat_index = jnp.arange(N_COL * N_ROW, dtype=jnp.int32).reshape(N_COL, N_ROW)
    return jnp.where(flat_index == hub_index, TMAX, base_count).astype(jnp.int32)


def draw_diagonal(key, part):
    position = jnp.arange(ORDER, dtype=jnp.float32) / ORDER
    ramp = jnp.exp(math.log(3.0) * position)
    rough = jnp.exp(jax.random.uniform(key, (ORDER,), jnp.float32, 0.0, math.log(2.0)))
    return jnp.clip(ramp * rough, 1.0, 6.0)


def touch_ends(array, rng, smallest, largest):
    shape = array.shape
    place = [jax.random.randint(jax.random.fold_in(rng, axis), (), 0, shape[axis]) for axis in range(len(shape))]
    array = array.at[tuple(place)].set(smallest)
    longest = shape.index(max(shape))
    place[longest] = (place[longest] + 1) % shape[longest]
    return array.at[tuple(place)].set(largest)


def block_levels(stream_key, extent, shards, least, largest):
    def one(dim, shards_of):
        steps = jax.random.uniform(jax.random.fold_in(jax.random.fold_in(stream_key, 6), dim), (shards_of,), jnp.float32, least / len(shards), largest / len(shards))
        return jnp.repeat(jnp.exp(steps), extent[dim] // shards_of).reshape((-1,) + (1,) * (len(extent) - dim - 1))

    gain = one(*shards[0])
    for cut in shards[1:]:
        gain = gain * one(*cut)
    return gain


def rank_bounds(count, slope):
    portions = [(1 << 20) // math.isqrt(standing ** slope) + 1 for standing in range(1, count + 1)]
    width = 1 + sum(portions) // (1 << 30)
    return np.cumsum(np.array([max(1, weight // width) for weight in portions]))


def skewed_ids(stream_key, extent, amount, skew):
    listing = rank_bounds(amount, skew)
    ticket = jax.random.randint(jax.random.fold_in(stream_key, 1), extent, 0, int(listing[amount - 1]))
    rank = jnp.searchsorted(jnp.asarray(listing, jnp.int32), ticket, side="right")
    return jax.random.permutation(jax.random.fold_in(stream_key, 2), amount)[rank].astype(jnp.int32)


def gaussian(key, dims, width, reach, pieces=(), held_as=jnp.bfloat16):
    factor_of = block_levels(key, dims, pieces, -0.22, 0.18) if pieces else 1.0
    drawn = jax.random.normal(key, dims, jnp.float32) * width * factor_of
    return jnp.minimum(jnp.maximum(drawn, -reach), reach).astype(held_as)


def setup_inputs(seed: int = 0) -> dict:
    streams_of = jax.random.split(jax.random.key(seed), 7)
    return {
        "basis_blocks": draw_basis_blocks(jax.random.fold_in(streams_of[6], 71), 0),
        "tile_values": gaussian(streams_of[1], (N_COL, N_ROW, TMAX, TILE, TILE), 0.0625, 0.375, ((0, 8), (1, 16))),
        "tile_rows": touch_ends(jax.random.randint(streams_of[2], (N_COL, N_ROW, TMAX), 0, BLOCK_ROWS // 128), jax.random.fold_in(streams_of[2], 1), 0, (BLOCK_ROWS // 128) - 1).astype(jnp.int32),
        "tile_column": touch_ends(skewed_ids(streams_of[3], (N_COL, N_ROW, TMAX), BLOCK_COLS // 128, 2), jax.random.fold_in(streams_of[3], 3), 0, (BLOCK_COLS // 128) - 1).astype(jnp.int32),
        "tile_count": draw_tile_count(jax.random.fold_in(streams_of[6], 71), 0),
        "diagonal": draw_diagonal(jax.random.fold_in(streams_of[6], 71), 0),
    }


def reference(basis_blocks, tile_values, tile_rows, tile_column, tile_count, diagonal):
    col_count, row_count, tile_slots = tile_rows.shape
    rhs_width = basis_blocks.shape[1]
    total_rows = basis_blocks.shape[2]
    seg_rows = total_rows // (col_count * row_count)
    block_tiles = row_count * seg_rows // 128
    vector = basis_blocks[-1].astype(jnp.bfloat16)
    per_set = vector.reshape(rhs_width, col_count, row_count, seg_rows).transpose(2, 0, 1, 3)
    per_set = per_set.reshape(row_count, rhs_width, col_count * seg_rows // 128, 128)

    def one_block(col_index):

        def add_part(accumulated, row_index):
            xblocks = per_set[row_index]
            gathered = jnp.take(xblocks, tile_column[col_index, row_index], axis=1)
            products = jnp.einsum('stj,tji->tsi', gathered.astype(jnp.float32), tile_values[col_index, row_index].astype(jnp.float32))
            live_tiles = (jnp.arange(tile_slots, dtype=jnp.int32) < tile_count[col_index, row_index]).astype(jnp.float32)
            products = products * live_tiles[:, None, None]
            summed = jax.ops.segment_sum(products, tile_rows[col_index, row_index], num_segments=block_tiles)
            return (accumulated + summed, None)
        initial = jnp.zeros((block_tiles, rhs_width, 128), jnp.float32)
        result, unused = lax.scan(add_part, initial, jnp.arange(row_count, dtype=jnp.int32))
        return result
    blocks_out = lax.map(one_block, jnp.arange(col_count, dtype=jnp.int32))
    image_rows = blocks_out.transpose(2, 0, 1, 3).reshape(rhs_width, total_rows)
    image_rows = image_rows + diagonal[None, :] * basis_blocks[-1]
    highest = lax.Precision.HIGHEST
    coefficients = jnp.einsum('kap,bp->kab', basis_blocks, image_rows, precision=highest) / total_rows
    projected = image_rows - jnp.einsum('kab,kap->bp', coefficients, basis_blocks, precision=highest)
    gram_matrix = jnp.dot(projected, projected.T, precision=highest) / total_rows
    lower_factor = jnp.linalg.cholesky(gram_matrix)
    new_block = lax.linalg.triangular_solve(lower_factor, projected, left_side=True, lower=True)
    return (new_block, coefficients, lower_factor.T)
```

```python
import functools

import jax
import jax.numpy as jnp
from jax import lax
from jax.experimental import pallas as pl
from jax.experimental.pallas import tpu as pltpu
from jax.sharding import Mesh
from jax.sharding import PartitionSpec as P

X, Z, Y, K = "row_0", "row_1", "col_0", "col_1"
ROW = (X, Z)
COL = (Y, K)
COL_ROW = (Y, K, X, Z)
MESH = pl.DeviceIdType.MESH
F32, BF16 = jnp.float32, jnp.bfloat16
NT = (((1,), (1,)), ((), ()))
CHUNK = 1024


def send(src, dst, send_sem, recv_sem, **to):
    return pltpu.make_async_remote_copy(
        src_ref=src, dst_ref=dst, send_sem=send_sem, recv_sem=recv_sem, device_id=to, device_id_type=MESH
    )


def halves(value):
    high = value.astype(BF16)
    return high, (value - high.astype(F32)).astype(BF16)


def dot(a, b, dims=(((1,), (0,)), ((), ()))):
    return lax.dot_general(a, b, dims, preferred_element_type=F32)


def lanes(m):
    return pl.ds(pl.multiple_of(m * 128, 128), 128)


def kernel(
    total_rows,
    cols_ref, prev_ref, last_ref, basis_hbm, tiles_hbm, diag_ref,
    out_ref, coef_ref, tri_ref,
    basis, tiles, xg, chain, qh, ql, w,
    sb1, rb1, sb2, rb2, zside, zown,
    inner, outer,
    load_sem, ag_send, ag_recv, rs_send, rs_recv, ar_send, ar_recv,
):
    x0, z0, y0, k0 = (lax.axis_index(a) for a in (X, Z, Y, K))
    blocks, rhs, seg = basis.shape
    slots = tiles.shape[0]
    seg_tiles = seg // 128
    part = seg_tiles // 2
    quarter = part // 2
    c0 = y0 * 2 + k0
    r0 = x0 * 4 + z0

    load_vector = pltpu.make_async_copy(basis_hbm.at[blocks - 1], basis.at[blocks - 1], load_sem.at[0])
    load_basis = pltpu.make_async_copy(
        basis_hbm.at[pl.ds(0, blocks - 1)], basis.at[pl.ds(0, blocks - 1)], load_sem.at[1]
    )
    load_vector.start()
    load_basis.start()
    piece = slots // 4
    loads = [
        pltpu.make_async_copy(
            tiles_hbm.at[pl.ds(i * piece, piece)], tiles.at[pl.ds(i * piece, piece)], load_sem.at[2 + i]
        )
        for i in range(4)
    ]
    for copy in loads:
        copy.start()

    barrier = pltpu.get_barrier_semaphore()
    inner_peers = [lax.rem(c0 + d, 8) for d in range(1, 8)]
    outer_peers = [lax.rem(r0 + d, 16) for d in range(1, 16)]
    for p in inner_peers:
        pl.semaphore_signal(barrier, inc=1, device_id={Y: p // 2, K: lax.rem(p, 2)}, device_id_type=MESH)
    for p in outer_peers:
        pl.semaphore_signal(barrier, inc=1, device_id={X: p // 4, Z: lax.rem(p, 4)}, device_id_type=MESH)

    load_vector.wait()
    own = c0 * seg_tiles

    def to_tiles(m, _):
        xg[own + m] = basis[blocks - 1, :, lanes(m)].astype(BF16)
        return 0

    lax.fori_loop(0, seg_tiles, to_tiles, 0, unroll=8)
    pl.semaphore_wait(barrier, 22)

    up, down, far = lax.rem(y0 + 1, 4), lax.rem(y0 + 3, 4), lax.rem(y0 + 2, 4)

    def chunk(y, k, h):
        return xg.at[pl.ds((y * 2 + k) * seg_tiles + h * part, part)]

    def hop(i, y, h, to):
        ref = chunk(y, k0, h)
        return send(ref, ref, ag_send.at[i], ag_recv.at[i], **{Y: to})

    def across(i, y, h, k):
        ref = chunk(y, k, h)
        return send(ref, ref, ag_send.at[6 + i], ag_recv.at[6 + i], **{K: 1 - k0})

    hops = [hop(0, y0, 0, up), hop(1, y0, 1, up), hop(2, y0, 1, down), hop(3, y0, 0, down)]
    for i in (0, 2, 1, 3):
        hops[i].start()
    arrive = [
        hop(0, down, 0, up), hop(1, down, 1, up), hop(2, up, 1, down),
        hop(3, up, 0, down), hop(4, far, 0, up), hop(5, far, 1, down),
    ]
    over = [across(i * 2 + h, y, h, k0) for i, y in enumerate((y0, down, up, far)) for h in range(2)]
    over[0].start()
    over[1].start()

    load_basis.wait()

    def split_basis(i, _):
        at = pl.ds(pl.multiple_of(i * CHUNK, CHUNK), CHUNK)
        for k in range(blocks):
            high, low = halves(basis[k, :, at])
            qh[pl.ds(k * rhs, rhs), at] = high
            ql[pl.ds(k * rhs, rhs), at] = low
        w[:, at] = basis[blocks - 1, :, at] * diag_ref[:, at]
        return 0

    lax.fori_loop(0, seg // CHUNK, split_basis, 0)

    arrive[0].wait_recv()
    forward_up = hop(4, down, 0, up)
    forward_up.start()
    over[2].start()
    arrive[2].wait_recv()
    forward_down = hop(5, up, 1, down)
    forward_down.start()
    over[5].start()
    for i, j in ((1, 3), (3, 4), (4, 6), (5, 7)):
        arrive[i].wait_recv()
        over[j].start()
    for i, y in enumerate((y0, down, up, far)):
        for h in range(2):
            across(i * 2 + h, y, h, 1 - k0).wait_recv()
    for copy in loads:
        copy.wait()

    chain[0] = jnp.zeros((rhs, 128), F32)
    step = 16

    def products(i, _):
        base = i * step
        made = [dot(xg[cols_ref[base + j]], tiles[base + j]) for j in range(step)]
        for j in range(step):
            chain[base + j + 1] = made[j] + chain[prev_ref[base + j]]
        return 0

    lax.fori_loop(0, slots // step, products, 0)

    for copy in hops + over + [forward_up, forward_down]:
        copy.wait_send()

    first = ((X, x0), (Z, z0))
    second = ((Z, z0), (X, x0))

    def near(pos, d):
        return lax.rem(pos + d, 4)

    def partial(half, f, g, m):
        r = f * 4 + g if half == 0 else g * 4 + f
        return chain[last_ref[r * seg_tiles + half * part + m]]

    def hop1(half, i):
        axis, pos = first[half]
        return send(
            sb1.at[half, i], rb1.at[half, i], rs_send.at[half, i], rs_recv.at[half, i],
            **{axis: near(pos, 1 if i % 2 == 0 else 3)},
        )

    def hop2(half, i):
        axis, pos = second[half]
        return send(
            sb2.at[half, i], rb2.at[half, i], rs_send.at[half, 6 + i], rs_recv.at[half, 6 + i],
            **{axis: near(pos, 1 if i % 2 == 0 else 3)},
        )

    def fill1(half, i, f, h, arrived=None):
        def body(m, _):
            for g in range(2):
                value = partial(half, f, 2 * h + g, m)
                if arrived is not None:
                    value = value + rb1[half, arrived, g * part + m].astype(F32)
                sb1[half, i, g * part + m] = value.astype(BF16)
            return 0

        lax.fori_loop(0, part, body, 0, unroll=8)
        hop1(half, i).start()

    for half in range(2):
        f0 = first[half][1]
        fill1(half, 0, near(f0, 2), 0)
        fill1(half, 1, near(f0, 2), 1)
    for half in range(2):
        f0 = first[half][1]
        fill1(half, 2, near(f0, 1), 1)
        fill1(half, 3, near(f0, 3), 0)
    for half in range(2):
        f0 = first[half][1]
        hop1(half, 0).wait_recv()
        fill1(half, 4, near(f0, 1), 0, 0)
        hop1(half, 1).wait_recv()
        fill1(half, 5, near(f0, 3), 1, 1)

    def summed1(half, g, m):
        h = g // 2
        at = (g - 2 * h) * part + m
        return (
            partial(half, first[half][1], g, m)
            + rb1[half, 3 - h, at].astype(F32)
            + rb1[half, 4 + h, at].astype(F32)
        )

    def over_part(body):
        lax.fori_loop(0, quarter, lambda m, _: (body(m), 0)[1], 0, unroll=8)

    for half in range(2):
        g0 = second[half][1]
        for i in range(2, 6):
            hop1(half, i).wait_recv()

        def far_block(m):
            sb2[half, 0, m] = summed1(half, near(g0, 2), m).astype(BF16)
            sb2[half, 1, m] = summed1(half, near(g0, 2), quarter + m).astype(BF16)

        over_part(far_block)
        hop2(half, 0).start()
        hop2(half, 1).start()

        def near_block(m):
            sb2[half, 2, m] = summed1(half, near(g0, 1), quarter + m).astype(BF16)
            sb2[half, 3, m] = summed1(half, near(g0, 3), m).astype(BF16)

        over_part(near_block)
        hop2(half, 2).start()
        hop2(half, 3).start()

        def kept(m):
            zside[half, 0, m] = summed1(half, near(g0, 1), m)
            zside[half, 1, m] = summed1(half, near(g0, 3), quarter + m)
            zown[half, m] = summed1(half, g0, m)
            zown[half, quarter + m] = summed1(half, g0, quarter + m)

        over_part(kept)
    for half in range(2):
        hop2(half, 0).wait_recv()
        hop2(half, 1).wait_recv()

        def joined(m):
            sb2[half, 4, m] = (zside[half, 0, m] + rb2[half, 0, m].astype(F32)).astype(BF16)
            sb2[half, 5, m] = (zside[half, 1, m] + rb2[half, 1, m].astype(F32)).astype(BF16)

        over_part(joined)
        hop2(half, 4).start()
        hop2(half, 5).start()
    for half in range(2):
        for i in range(2, 6):
            hop2(half, i).wait_recv()

        def arrived_rows(m):
            low = lanes(half * part + m)
            w[:, low] = w[:, low] + (
                zown[half, m] + rb2[half, 3, m].astype(F32) + rb2[half, 4, m].astype(F32)
            )
            high = lanes(half * part + quarter + m)
            w[:, high] = w[:, high] + (
                zown[half, quarter + m] + rb2[half, 2, m].astype(F32) + rb2[half, 5, m].astype(F32)
            )

        over_part(arrived_rows)

    def total(value, use):
        def inner_copy(d):
            p = lax.rem(c0 + d, 8)
            mine = inner.at[use, c0]
            return send(
                mine, mine, ar_send.at[use, d], ar_recv.at[use, d], **{Y: p // 2, K: lax.rem(p, 2)}
            )

        def outer_copy(d):
            p = lax.rem(r0 + d, 16)
            mine = outer.at[use, r0]
            return send(
                mine, mine, ar_send.at[use, 8 + d], ar_recv.at[use, 8 + d], **{X: p // 4, Z: lax.rem(p, 4)}
            )

        inner[use, c0] = value
        for d in range(1, 8):
            inner_copy(d).start()
        for d in range(1, 8):
            inner_copy(d).wait_recv()
        acc = inner[use, 0]
        for i in range(1, 8):
            acc = acc + inner[use, i]
        outer[use, r0] = acc
        for d in range(1, 16):
            outer_copy(d).start()
        for d in range(1, 16):
            outer_copy(d).wait_recv()
        acc = outer[use, 0]
        for i in range(1, 16):
            acc = acc + outer[use, i]
        for d in range(1, 8):
            inner_copy(d).wait_send()
        for d in range(1, 16):
            outer_copy(d).wait_send()
        return acc * F32(1.0 / total_rows)

    def project(i, acc):
        at = pl.ds(pl.multiple_of(i * CHUNK, CHUNK), CHUNK)
        high, low = halves(w[:, at])
        both = dot(jnp.concatenate([high, low], axis=0), qh[:, at], NT)
        return acc + (both[:rhs] + both[rhs:] + dot(high, ql[:, at], NT))

    coef = total(lax.fori_loop(0, seg // CHUNK, project, jnp.zeros((rhs, blocks * rhs), F32)), 0)
    coef_ref[...] = coef
    coef_high, coef_low = halves(coef)
    coef_both = jnp.concatenate([coef_high, coef_low], axis=0)

    def subtract(i, acc):
        at = pl.ds(pl.multiple_of(i * CHUNK, CHUNK), CHUNK)
        both = dot(coef_both, qh[:, at])
        rest = w[:, at] - (both[:rhs] + both[rhs:] + dot(coef_high, ql[:, at]))
        w[:, at] = rest
        high, low = halves(rest)
        both = dot(jnp.concatenate([high, low], axis=0), high, NT)
        return acc + (both[:rhs] + both[rhs:] + dot(high, low, NT))

    gram = lax.fori_loop(0, seg // CHUNK, subtract, jnp.zeros((rhs, rhs), F32))
    gram = total(jnp.concatenate([gram, jnp.zeros((rhs, 128 - rhs), F32)], axis=1), 1)

    row = lax.broadcasted_iota(jnp.int32, (rhs, 128), 0)
    lane = lax.broadcasted_iota(jnp.int32, (rhs, 128), 1)
    m = jnp.where(lane < rhs, gram, jnp.where(lane - rhs == row, F32(1), F32(0)))
    for k in range(rhs - 1):
        factor = jnp.where(row[:, :1] > k, m[:, k : k + 1] / m[k : k + 1, k : k + 1], F32(0))
        m = m - factor * m[k : k + 1, :]
    pivots = jnp.sum(jnp.where(lane == row, m, F32(0)), axis=1, keepdims=True)
    m = m / jnp.sqrt(pivots)
    tri_ref[...] = jnp.where(lane >= row, m, F32(0))[:, :rhs]
    inv_high, inv_low = halves(m[:, rhs : 2 * rhs])
    inv_both = jnp.concatenate([inv_high, inv_low], axis=0)

    def solve(i, _):
        at = pl.ds(pl.multiple_of(i * CHUNK, CHUNK), CHUNK)
        high, low = halves(w[:, at])
        both = dot(inv_both, high)
        out_ref[:, at] = both[:rhs] + both[rhs:] + dot(inv_high, low)
        return 0

    lax.fori_loop(0, seg // CHUNK, solve, 0)
    for half in range(2):
        for i in range(6):
            hop1(half, i).wait_send()
            hop2(half, i).wait_send()


def local(basis_blocks, tile_values, tile_rows, tile_column, tile_count, diagonal):
    blocks, rhs, seg = basis_blocks.shape
    slots = tile_values.shape[2]
    seg_tiles = seg // 128
    part = seg_tiles // 2
    total_rows = seg * 128
    block_tiles = seg_tiles * 16

    slot = jnp.arange(slots, dtype=jnp.int32)
    live = slot < tile_count[0, 0]
    rows = jnp.where(live, tile_rows[0, 0], -1)
    cols = jnp.where(live, tile_column[0, 0], 0)
    earlier = (rows[:, None] == rows[None, :]) & (slot[:, None] < slot[None, :])
    prev = jnp.max(jnp.where(earlier, slot[:, None] + 1, 0), axis=0)
    hit = rows[:, None] == jnp.arange(block_tiles, dtype=jnp.int32)[None, :]
    last = jnp.max(jnp.where(hit, slot[:, None] + 1, 0), axis=0)

    smem = pl.BlockSpec(memory_space=pltpu.SMEM)
    vmem = pl.BlockSpec(memory_space=pltpu.VMEM)
    hbm = pl.BlockSpec(memory_space=pl.ANY)
    dma = pltpu.SemaphoreType.DMA
    tile = (rhs, 128)
    new_block, coef, triangle = pl.pallas_call(
        functools.partial(kernel, total_rows),
        out_shape=(
            jax.ShapeDtypeStruct((rhs, seg), F32),
            jax.ShapeDtypeStruct((rhs, blocks * rhs), F32),
            jax.ShapeDtypeStruct((rhs, rhs), F32),
        ),
        in_specs=[smem, smem, smem, hbm, hbm, vmem],
        out_specs=(vmem, vmem, vmem),
        scratch_shapes=[
            pltpu.VMEM((blocks, rhs, seg), F32),
            pltpu.VMEM((slots, 128, 128), BF16),
            pltpu.VMEM((8 * seg_tiles, *tile), BF16),
            pltpu.VMEM((slots + 8, *tile), F32),
            pltpu.VMEM((blocks * rhs, seg), BF16),
            pltpu.VMEM((blocks * rhs, seg), BF16),
            pltpu.VMEM((rhs, seg), F32),
            pltpu.VMEM((2, 6, 2 * part, *tile), BF16),
            pltpu.VMEM((2, 6, 2 * part, *tile), BF16),
            pltpu.VMEM((2, 6, part // 2, *tile), BF16),
            pltpu.VMEM((2, 6, part // 2, *tile), BF16),
            pltpu.VMEM((2, 2, part // 2, *tile), F32),
            pltpu.VMEM((2, part, *tile), F32),
            pltpu.VMEM((2, 8, *tile), F32),
            pltpu.VMEM((2, 16, *tile), F32),
            dma((6,)),
            dma((14,)),
            dma((14,)),
            dma((2, 12)),
            dma((2, 12)),
            dma((2, 24)),
            dma((2, 24)),
        ],
        compiler_params=pltpu.CompilerParams(
            collective_id=0, has_side_effects=True, vmem_limit_bytes=58 * 1024 * 1024
        ),
        name="step",
    )(cols, prev, last, basis_blocks, tile_values[0, 0], diagonal[None, :])
    return new_block, coef.T.reshape(blocks, rhs, rhs), triangle


def solution(mesh):
    split = Mesh(mesh.devices.reshape(4, 4, 4, 2), (X, Z, Y, K))
    placed = (
        P(None, None, COL_ROW),
        P(COL, ROW, None, None, None),
        P(COL, ROW, None),
        P(COL, ROW, None),
        P(COL, ROW),
        P(COL_ROW),
    )
    return jax.shard_map(
        local, mesh=split, in_specs=placed, out_specs=(P(None, COL_ROW), P(), P()), check_vma=False
    )
```

```python
import functools

import jax
import jax.numpy as jnp
from jax import lax
from jax.experimental import pallas as pl
from jax.experimental.pallas import tpu as pltpu
from jax.sharding import Mesh
from jax.sharding import PartitionSpec as P

X, Z, Y, K = "row_0", "row_1", "col_0", "col_1"
ROW = (X, Z)
COL = (Y, K)
COL_ROW = (Y, K, X, Z)
MESH = pl.DeviceIdType.MESH
F32, BF16 = jnp.float32, jnp.bfloat16
NT = (((1,), (1,)), ((), ()))
CHUNK = 1024


def send(src, dst, send_sem, recv_sem, **to):
    return pltpu.make_async_remote_copy(
        src_ref=src, dst_ref=dst, send_sem=send_sem, recv_sem=recv_sem, device_id=to, device_id_type=MESH
    )


def halves(value):
    high = value.astype(BF16)
    return high, (value - high.astype(F32)).astype(BF16)


def dot(a, b, dims=(((1,), (0,)), ((), ()))):
    return lax.dot_general(a, b, dims, preferred_element_type=F32)


def lanes(m):
    return pl.ds(pl.multiple_of(m * 128, 128), 128)


def kernel(
    total_rows,
    count_ref, cols_ref, rows_ref, basis_hbm, tiles_hbm, diag_ref,
    out_ref, coef_ref, tri_ref,
    basis, tiles, xg, chain, q2, w,
    sb1, rb1, sb2, rb2, zside, zown,
    prev_vec, last_vec, prev_ref, last_ref,
    mine, pair, ring, whole, inner, outer,
    load_sem, ag_send, ag_recv, rs_send, rs_recv, ea_send, ea_recv, ar_send, ar_recv,
):
    x0, z0, y0, k0 = (lax.axis_index(a) for a in (X, Z, Y, K))
    blocks, rhs, seg = basis.shape
    slots = tiles.shape[0]
    seg_tiles = seg // 128
    part = seg_tiles // 2
    quarter = part // 2
    c0 = y0 * 2 + k0
    r0 = x0 * 4 + z0

    load_vector = pltpu.make_async_copy(basis_hbm.at[blocks - 1], basis.at[blocks - 1], load_sem.at[0])
    load_basis = pltpu.make_async_copy(
        basis_hbm.at[pl.ds(0, blocks - 1)], basis.at[pl.ds(0, blocks - 1)], load_sem.at[1]
    )
    load_vector.start()
    load_basis.start()
    piece = slots // 4
    loads = [
        pltpu.make_async_copy(
            tiles_hbm.at[pl.ds(i * piece, piece)], tiles.at[pl.ds(i * piece, piece)], load_sem.at[2 + i]
        )
        for i in range(4)
    ]
    for copy in loads:
        copy.start()

    barrier = pltpu.get_barrier_semaphore()
    inner_peers = [lax.rem(c0 + d, 8) for d in range(1, 8)]
    outer_peers = [lax.rem(r0 + d, 16) for d in range(1, 16)]
    for p in inner_peers:
        pl.semaphore_signal(barrier, inc=1, device_id={Y: p // 2, K: lax.rem(p, 2)}, device_id_type=MESH)
    for p in outer_peers:
        pl.semaphore_signal(barrier, inc=1, device_id={X: p // 4, Z: lax.rem(p, 4)}, device_id_type=MESH)

    load_vector.wait()
    own = c0 * seg_tiles

    def to_tiles(m, _):
        xg[own + m] = basis[blocks - 1, :, lanes(m)].astype(BF16)
        return 0

    lax.fori_loop(0, seg_tiles, to_tiles, 0, unroll=8)
    pl.semaphore_wait(barrier, 22)

    up, down, far = lax.rem(y0 + 1, 4), lax.rem(y0 + 3, 4), lax.rem(y0 + 2, 4)

    def chunk(y, k, h):
        return xg.at[pl.ds((y * 2 + k) * seg_tiles + h * part, part)]

    def hop(i, y, h, to):
        ref = chunk(y, k0, h)
        return send(ref, ref, ag_send.at[i], ag_recv.at[i], **{Y: to})

    def across(i, y, h, k):
        ref = chunk(y, k, h)
        return send(ref, ref, ag_send.at[6 + i], ag_recv.at[6 + i], **{K: 1 - k0})

    hops = [hop(0, y0, 0, up), hop(1, y0, 1, up), hop(2, y0, 1, down), hop(3, y0, 0, down)]
    for i in (0, 2, 1, 3):
        hops[i].start()
    arrive = [
        hop(0, down, 0, up), hop(1, down, 1, up), hop(2, up, 1, down),
        hop(3, up, 0, down), hop(4, far, 0, up), hop(5, far, 1, down),
    ]
    over = [across(i * 2 + h, y, h, k0) for i, y in enumerate((y0, down, up, far)) for h in range(2)]
    over[0].start()
    over[1].start()

    load_basis.wait()

    width = blocks * rhs

    def split_basis(i, acc):
        at = pl.ds(pl.multiple_of(i * CHUNK, CHUNK), CHUNK)
        for k in range(blocks):
            high, low = halves(basis[k, :, at])
            q2[pl.ds(k * rhs, rhs), at] = high
            q2[pl.ds(width + k * rhs, rhs), at] = low
        shifted = basis[blocks - 1, :, at] * diag_ref[:, at]
        w[:, at] = shifted
        stack = jnp.concatenate([q2[:, at], shifted.astype(BF16)], axis=0)
        return acc + dot(stack, q2[pl.ds(0, width), at], NT)

    made = lax.fori_loop(0, seg // CHUNK, split_basis, jnp.zeros((2 * width + rhs, width), F32))
    mine[pl.ds(0, width)] = made[:width] + made[width : 2 * width] + made[width : 2 * width].T
    mine[pl.ds(width, rhs)] = made[2 * width :]

    load = (width + rhs) // 2
    ring_axes = ((X, x0), (Z, z0), (Y, y0))
    to_pair = send(
        mine.at[pl.ds(pl.multiple_of((1 - k0) * load, 8), load)], pair, ea_send.at[0], ea_recv.at[0], **{K: 1 - k0}
    )
    to_pair.start()

    def ring_copy(i, d):
        axis, pos = ring_axes[i]
        ref = ring.at[i, pos]
        return send(ref, ref, ea_send.at[3 * i + d], ea_recv.at[3 * i + d], **{axis: lax.rem(pos + d, 4)})

    def ring_start(i, value):
        ring[i, ring_axes[i][1]] = value
        for d in range(1, 4):
            ring_copy(i, d).start()

    def ring_sum(i):
        for d in range(1, 4):
            ring_copy(i, d).wait_recv()
        return (ring[i, 0] + ring[i, 1]) + (ring[i, 2] + ring[i, 3])

    lane_slot = lax.broadcasted_iota(jnp.int32, (1, 128), 1)
    sub_slot = lax.broadcasted_iota(jnp.int32, (128, 128), 0)
    count = count_ref[0, 0]
    row_lanes, row_subs = [], []
    for c in range(slots // 128):
        row_c = rows_ref[:, pl.ds(c * 128, 128)]
        row_c = jnp.where(lane_slot + c * 128 < count, row_c, -1)
        row_lanes.append(row_c)
        row_subs.append(jnp.broadcast_to(row_c, (128, 128)).T)
    for c in range(slots // 128):
        best = jnp.zeros((1, 128), jnp.int32)
        for e in range(c + 1):
            found = row_subs[e] == row_lanes[c]
            if e == c:
                found = found & (sub_slot < lane_slot)
            best = jnp.maximum(best, jnp.max(jnp.where(found, sub_slot + (e * 128 + 1), 0), axis=0, keepdims=True))
        prev_vec[:, pl.ds(c * 128, 128)] = best
    for c in range(last_vec.shape[1] // 128):
        best = jnp.zeros((1, 128), jnp.int32)
        for e in range(slots // 128):
            found = row_subs[e] == lane_slot + c * 128
            best = jnp.maximum(best, jnp.max(jnp.where(found, sub_slot + (e * 128 + 1), 0), axis=0, keepdims=True))
        last_vec[:, pl.ds(c * 128, 128)] = best
    tables = [
        pltpu.make_async_copy(prev_vec, prev_ref, load_sem.at[6]),
        pltpu.make_async_copy(last_vec, last_ref, load_sem.at[7]),
    ]
    for copy in tables:
        copy.start()

    arrive[0].wait_recv()
    forward_up = hop(4, down, 0, up)
    forward_up.start()
    over[2].start()
    to_pair.wait_recv()
    ring_start(0, mine[pl.ds(pl.multiple_of(k0 * load, 8), load)] + pair[...])
    arrive[2].wait_recv()
    forward_down = hop(5, up, 1, down)
    forward_down.start()
    over[5].start()
    for i, j in ((1, 3), (3, 4)):
        arrive[i].wait_recv()
        over[j].start()
    ring_start(1, ring_sum(0))
    for i, j in ((4, 6), (5, 7)):
        arrive[i].wait_recv()
        over[j].start()
    ring_start(2, ring_sum(1))
    for i, y in enumerate((y0, down, up, far)):
        for h in range(2):
            across(i * 2 + h, y, h, 1 - k0).wait_recv()
    for copy in loads + tables:
        copy.wait()

    chain[0] = jnp.zeros((rhs, 128), F32)
    step = 16

    def products(i, _):
        base = i * step
        made = [dot(xg[jnp.clip(cols_ref[0, 0, base + j], 0, 8 * seg_tiles - 1)], tiles[base + j]) for j in range(step)]
        for j in range(step):
            chain[base + j + 1] = made[j] + chain[prev_ref[0, base + j]]
        return 0

    lax.fori_loop(0, slots // step, products, 0)

    for copy in hops + over + [forward_up, forward_down]:
        copy.wait_send()

    first = ((X, x0), (Z, z0))
    second = ((Z, z0), (X, x0))

    def near(pos, d):
        return lax.rem(pos + d, 4)

    def partial(half, f, g, m):
        r = f * 4 + g if half == 0 else g * 4 + f
        return chain[last_ref[0, r * seg_tiles + half * part + m]]

    def hop1(half, i):
        axis, pos = first[half]
        return send(
            sb1.at[half, i], rb1.at[half, i], rs_send.at[half, i], rs_recv.at[half, i],
            **{axis: near(pos, 1 if i % 2 == 0 else 3)},
        )

    def hop2(half, i):
        axis, pos = second[half]
        return send(
            sb2.at[half, i], rb2.at[half, i], rs_send.at[half, 6 + i], rs_recv.at[half, 6 + i],
            **{axis: near(pos, 1 if i % 2 == 0 else 3)},
        )

    def fill1(half, i, f, h, arrived=None):
        def body(m, _):
            for g in range(2):
                value = partial(half, f, 2 * h + g, m)
                if arrived is not None:
                    value = value + rb1[half, arrived, g * part + m].astype(F32)
                sb1[half, i, g * part + m] = value.astype(BF16)
            return 0

        lax.fori_loop(0, part, body, 0, unroll=8)
        hop1(half, i).start()

    for half in range(2):
        f0 = first[half][1]
        fill1(half, 0, near(f0, 2), 0)
        fill1(half, 1, near(f0, 2), 1)
    for half in range(2):
        f0 = first[half][1]
        fill1(half, 2, near(f0, 1), 1)
        fill1(half, 3, near(f0, 3), 0)
    whole[k0] = ring_sum(2) * F32(1.0 / total_rows)
    back = send(whole.at[k0], whole.at[k0], ea_send.at[10], ea_recv.at[10], **{K: 1 - k0})
    back.start()
    for half in range(2):
        f0 = first[half][1]
        hop1(half, 0).wait_recv()
        fill1(half, 4, near(f0, 1), 0, 0)
        hop1(half, 1).wait_recv()
        fill1(half, 5, near(f0, 3), 1, 1)

    def summed1(half, g, m):
        h = g // 2
        at = (g - 2 * h) * part + m
        return (
            partial(half, first[half][1], g, m)
            + rb1[half, 3 - h, at].astype(F32)
            + rb1[half, 4 + h, at].astype(F32)
        )

    def over_part(body):
        lax.fori_loop(0, quarter, lambda m, _: (body(m), 0)[1], 0, unroll=8)

    back.wait_recv()
    products_of = jnp.concatenate([whole[0], whole[1]], axis=0)
    basis_gram = products_of[:width]
    guess = products_of[width:]
    exact = lax.Precision.HIGHEST

    def full(a, b, dims=(((1,), (0,)), ((), ()))):
        return lax.dot_general(a, b, dims, precision=exact, preferred_element_type=F32)

    guess_left = full(guess, basis_gram) - guess

    def paired(a):
        high, low = halves(a)
        top = jnp.concatenate([high, high], axis=1)
        return jnp.concatenate([top, jnp.concatenate([low, jnp.zeros_like(low)], axis=1)], axis=0)

    guess_pair = paired(guess)

    def lessen(i, _):
        at = pl.ds(pl.multiple_of(i * CHUNK, CHUNK), CHUNK)
        both = dot(guess_pair, q2[:, at])
        w[:, at] = w[:, at] - (both[:rhs] + both[rhs:])
        return 0

    lax.fori_loop(0, seg // CHUNK, lessen, 0)
    for half in range(2):
        g0 = second[half][1]
        for i in range(2, 6):
            hop1(half, i).wait_recv()

        def far_block(m):
            sb2[half, 0, m] = summed1(half, near(g0, 2), m).astype(BF16)
            sb2[half, 1, m] = summed1(half, near(g0, 2), quarter + m).astype(BF16)

        over_part(far_block)
        hop2(half, 0).start()
        hop2(half, 1).start()

        def near_block(m):
            sb2[half, 2, m] = summed1(half, near(g0, 1), quarter + m).astype(BF16)
            sb2[half, 3, m] = summed1(half, near(g0, 3), m).astype(BF16)

        over_part(near_block)
        hop2(half, 2).start()
        hop2(half, 3).start()

        def kept(m):
            zside[half, 0, m] = summed1(half, near(g0, 1), m)
            zside[half, 1, m] = summed1(half, near(g0, 3), quarter + m)
            zown[half, m] = summed1(half, g0, m)
            zown[half, quarter + m] = summed1(half, g0, quarter + m)

        over_part(kept)
    for half in range(2):
        hop2(half, 0).wait_recv()
        hop2(half, 1).wait_recv()

        def joined(m):
            sb2[half, 4, m] = (zside[half, 0, m] + rb2[half, 0, m].astype(F32)).astype(BF16)
            sb2[half, 5, m] = (zside[half, 1, m] + rb2[half, 1, m].astype(F32)).astype(BF16)

        over_part(joined)
        hop2(half, 4).start()
        hop2(half, 5).start()
    for half in range(2):
        for i in range(2, 6):
            hop2(half, i).wait_recv()

        def arrived_rows(m):
            low = lanes(half * part + m)
            w[:, low] = w[:, low] + (
                zown[half, m] + rb2[half, 3, m].astype(F32) + rb2[half, 4, m].astype(F32)
            )
            high = lanes(half * part + quarter + m)
            w[:, high] = w[:, high] + (
                zown[half, quarter + m] + rb2[half, 2, m].astype(F32) + rb2[half, 5, m].astype(F32)
            )

        over_part(arrived_rows)

    def inner_copy(d):
        p = lax.rem(c0 + d, 8)
        ref = inner.at[c0]
        return send(ref, ref, ar_send.at[d], ar_recv.at[d], **{Y: p // 2, K: lax.rem(p, 2)})

    def outer_copy(d):
        p = lax.rem(r0 + d, 16)
        ref = outer.at[r0]
        return send(ref, ref, ar_send.at[8 + d], ar_recv.at[8 + d], **{X: p // 4, Z: lax.rem(p, 4)})

    def project(i, acc):
        at = pl.ds(pl.multiple_of(i * CHUNK, CHUNK), CHUNK)
        stack = jnp.concatenate(halves(w[:, at]), axis=0)
        return acc[0] + dot(stack, q2[:, at], NT), acc[1] + dot(stack, stack, NT)

    with_basis, with_self = lax.fori_loop(
        0, seg // CHUNK, project, (jnp.zeros((2 * rhs, 2 * width), F32), jnp.zeros((2 * rhs, 2 * rhs), F32))
    )
    inner[c0, pl.ds(0, rhs)] = with_basis[:rhs, :width] + with_basis[rhs:, :width] + with_basis[:rhs, width:]
    with_self = with_self[:rhs, :rhs] + with_self[rhs:, :rhs] + with_self[:rhs, rhs:]
    inner[c0, pl.ds(rhs, rhs)] = jnp.concatenate([with_self, jnp.zeros((rhs, 128 - rhs), F32)], axis=1)
    for d in range(1, 8):
        inner_copy(d).start()
    for d in range(1, 8):
        inner_copy(d).wait_recv()
    acc = inner[0]
    for i in range(1, 8):
        acc = acc + inner[i]
    outer[r0] = acc
    for d in range(1, 16):
        outer_copy(d).start()
    for d in range(1, 16):
        outer_copy(d).wait_recv()
    acc = outer[0]
    for i in range(1, 16):
        acc = acc + outer[i]
    acc = acc * F32(1.0 / total_rows)
    reduced = acc[:rhs]
    rest = reduced + guess_left
    coef_ref[...] = rest + guess
    basis_gram = jnp.concatenate([whole[0], whole[1]], axis=0)[:width]
    turned = full(rest, basis_gram) - reduced
    cross = full(turned, rest, NT) - full(rest, reduced, NT)
    gram = acc[rhs:] + jnp.concatenate([cross, jnp.zeros((rhs, 128 - rhs), F32)], axis=1)

    row = lax.broadcasted_iota(jnp.int32, (rhs, 128), 0)
    lane = lax.broadcasted_iota(jnp.int32, (rhs, 128), 1)
    m = jnp.where(lane < rhs, gram, jnp.where(lane - rhs == row, F32(1), F32(0)))
    for k in range(rhs - 1):
        factor = jnp.where(row[:, :1] > k, m[:, k : k + 1] / m[k : k + 1, k : k + 1], F32(0))
        m = m - factor * m[k : k + 1, :]
    pivots = jnp.sum(jnp.where(lane == row, m, F32(0)), axis=1, keepdims=True)
    m = m / jnp.sqrt(pivots)
    tri_ref[...] = jnp.where(lane >= row, m, F32(0))[:, :rhs]
    inverse = m[:, rhs : 2 * rhs]
    back_pair = paired(-full(inverse, rest))
    inverse_pair = paired(inverse)

    def solve(i, _):
        at = pl.ds(pl.multiple_of(i * CHUNK, CHUNK), CHUNK)
        stack = jnp.concatenate(halves(w[:, at]), axis=0)
        both = dot(back_pair, q2[:, at]) + dot(inverse_pair, stack)
        out_ref[:, at] = both[:rhs] + both[rhs:]
        return 0

    lax.fori_loop(0, seg // CHUNK, solve, 0)
    for half in range(2):
        for i in range(6):
            hop1(half, i).wait_send()
            hop2(half, i).wait_send()
    for d in range(1, 8):
        inner_copy(d).wait_send()
    for d in range(1, 16):
        outer_copy(d).wait_send()
    to_pair.wait_send()
    back.wait_send()
    for i in range(3):
        for d in range(1, 4):
            ring_copy(i, d).wait_send()


def finish(block_in, coef_in, triangle_in, block_out, coef_out, triangle_out):
    block_out[...] = block_in[...]
    coef_out[...] = coef_in[...].T
    triangle_out[...] = triangle_in[...]


def local(basis_blocks, tile_values, tile_rows, tile_column, tile_count, diagonal):
    blocks, rhs, seg = basis_blocks.shape
    slots = tile_values.shape[2]
    seg_tiles = seg // 128
    part = seg_tiles // 2
    total_rows = seg * 128
    block_tiles = seg_tiles * 16

    smem = pl.BlockSpec(memory_space=pltpu.SMEM)
    vmem = pl.BlockSpec(memory_space=pltpu.VMEM)
    hbm = pl.BlockSpec(memory_space=pl.ANY)
    dma = pltpu.SemaphoreType.DMA
    tile = (rhs, 128)
    new_block, coef, triangle = pl.pallas_call(
        functools.partial(kernel, total_rows),
        out_shape=(
            jax.ShapeDtypeStruct((rhs, seg), F32),
            jax.ShapeDtypeStruct((rhs, blocks * rhs), F32),
            jax.ShapeDtypeStruct((rhs, rhs), F32),
        ),
        in_specs=[smem, smem, vmem, hbm, hbm, vmem],
        out_specs=(vmem, vmem, vmem),
        scratch_shapes=[
            pltpu.VMEM((blocks, rhs, seg), F32),
            pltpu.VMEM((slots, 128, 128), BF16),
            pltpu.VMEM((8 * seg_tiles, *tile), BF16),
            pltpu.VMEM((slots + 8, *tile), F32),
            pltpu.VMEM((2 * blocks * rhs, seg), BF16),
            pltpu.VMEM((rhs, seg), F32),
            pltpu.VMEM((2, 6, 2 * part, *tile), BF16),
            pltpu.VMEM((2, 6, 2 * part, *tile), BF16),
            pltpu.VMEM((2, 6, part // 2, *tile), BF16),
            pltpu.VMEM((2, 6, part // 2, *tile), BF16),
            pltpu.VMEM((2, 2, part // 2, *tile), F32),
            pltpu.VMEM((2, part, *tile), F32),
            pltpu.VMEM((1, slots), jnp.int32),
            pltpu.VMEM((1, block_tiles), jnp.int32),
            pltpu.SMEM((1, slots), jnp.int32),
            pltpu.SMEM((1, block_tiles), jnp.int32),
            pltpu.VMEM((9 * rhs, 128), F32),
            pltpu.VMEM((9 * rhs // 2, 128), F32),
            pltpu.VMEM((3, 4, 9 * rhs // 2, 128), F32),
            pltpu.VMEM((2, 9 * rhs // 2, 128), F32),
            pltpu.VMEM((8, 2 * rhs, 128), F32),
            pltpu.VMEM((16, 2 * rhs, 128), F32),
            dma((8,)),
            dma((14,)),
            dma((14,)),
            dma((2, 12)),
            dma((2, 12)),
            dma((11,)),
            dma((11,)),
            dma((24,)),
            dma((24,)),
        ],
        compiler_params=pltpu.CompilerParams(
            collective_id=0, has_side_effects=True, vmem_limit_bytes=58 * 1024 * 1024
        ),
        name="step",
    )(tile_count, tile_column, tile_rows[0], basis_blocks, tile_values[0, 0], diagonal[None, :])
    new_block, coef, triangle = pl.pallas_call(
        finish,
        out_shape=(
            jax.ShapeDtypeStruct((rhs, seg), F32),
            jax.ShapeDtypeStruct((blocks * rhs, rhs), F32),
            jax.ShapeDtypeStruct((rhs, rhs), F32),
        ),
        in_specs=[vmem] * 3,
        out_specs=(vmem,) * 3,
        name="finish",
    )(new_block, coef, triangle)
    return new_block, coef.reshape(blocks, rhs, rhs), triangle


def solution(mesh):
    split = Mesh(mesh.devices.reshape(4, 4, 4, 2), (X, Z, Y, K))
    placed = (
        P(None, None, COL_ROW),
        P(COL, ROW, None, None, None),
        P(COL, ROW, None),
        P(COL, ROW, None),
        P(COL, ROW),
        P(COL_ROW),
    )
    return jax.shard_map(
        local, mesh=split, in_specs=placed, out_specs=(P(None, COL_ROW), P(), P()), check_vma=False
    )
```

```python
import functools

import jax
import jax.numpy as jnp
from jax import lax
from jax.experimental import pallas as pl
from jax.experimental.pallas import tpu as pltpu
from jax.sharding import Mesh
from jax.sharding import PartitionSpec as P

X, Z, Y, K = "row_0", "row_1", "col_0", "col_1"
ROW = (X, Z)
COL = (Y, K)
COL_ROW = (Y, K, X, Z)
MESH = pl.DeviceIdType.MESH
F32, BF16 = jnp.float32, jnp.bfloat16
NT = (((1,), (1,)), ((), ()))
CHUNK = 1024


def send(src, dst, send_sem, recv_sem, **to):
    return pltpu.make_async_remote_copy(
        src_ref=src, dst_ref=dst, send_sem=send_sem, recv_sem=recv_sem, device_id=to, device_id_type=MESH
    )


def halves(value):
    high = value.astype(BF16)
    return high, (value - high.astype(F32)).astype(BF16)


def dot(a, b, dims=(((1,), (0,)), ((), ()))):
    return lax.dot_general(a, b, dims, preferred_element_type=F32)


def lanes(m):
    return pl.ds(pl.multiple_of(m * 128, 128), 128)


def kernel(
    total_rows,
    count_ref, cols_ref, rows_ref, basis_hbm, tiles_hbm, diag_ref,
    out_ref, coef_ref, tri_ref,
    basis, tiles, xg, chain, q2, qt, w,
    sb1, rb1, sb2, rb2, zside, zown,
    prev_vec, last_vec, prev_ref, last_ref,
    mine, pair, ring, whole, inner, outer,
    load_sem, ag_send, ag_recv, rs_send, rs_recv, ea_send, ea_recv, ar_send, ar_recv,
):
    x0, z0, y0, k0 = (lax.axis_index(a) for a in (X, Z, Y, K))
    blocks, rhs, seg = basis.shape
    slots = tiles.shape[0]
    seg_tiles = seg // 128
    part = seg_tiles // 2
    quarter = part // 2
    c0 = y0 * 2 + k0
    r0 = x0 * 4 + z0

    load_vector = pltpu.make_async_copy(basis_hbm.at[blocks - 1], basis.at[blocks - 1], load_sem.at[0])
    load_basis = pltpu.make_async_copy(
        basis_hbm.at[pl.ds(0, blocks - 1)], basis.at[pl.ds(0, blocks - 1)], load_sem.at[1]
    )
    load_vector.start()
    load_basis.start()
    piece = slots // 4
    loads = [
        pltpu.make_async_copy(
            tiles_hbm.at[pl.ds(i * piece, piece)], tiles.at[pl.ds(i * piece, piece)], load_sem.at[2 + i]
        )
        for i in range(4)
    ]
    for copy in loads:
        copy.start()

    barrier = pltpu.get_barrier_semaphore()
    inner_peers = [lax.rem(c0 + d, 8) for d in range(1, 8)]
    outer_peers = [lax.rem(r0 + d, 16) for d in range(1, 16)]
    for p in inner_peers:
        pl.semaphore_signal(barrier, inc=1, device_id={Y: p // 2, K: lax.rem(p, 2)}, device_id_type=MESH)
    for p in outer_peers:
        pl.semaphore_signal(barrier, inc=1, device_id={X: p // 4, Z: lax.rem(p, 4)}, device_id_type=MESH)

    load_vector.wait()
    own = c0 * seg_tiles

    def to_tiles(m, _):
        xg[own + m] = basis[blocks - 1, :, lanes(m)].astype(BF16)
        return 0

    lax.fori_loop(0, seg_tiles, to_tiles, 0, unroll=8)
    pl.semaphore_wait(barrier, 22)

    up, down, far = lax.rem(y0 + 1, 4), lax.rem(y0 + 3, 4), lax.rem(y0 + 2, 4)

    def chunk(y, k, h):
        return xg.at[pl.ds((y * 2 + k) * seg_tiles + h * part, part)]

    def hop(i, y, h, to):
        ref = chunk(y, k0, h)
        return send(ref, ref, ag_send.at[i], ag_recv.at[i], **{Y: to})

    def across(i, y, h, k):
        ref = chunk(y, k, h)
        return send(ref, ref, ag_send.at[6 + i], ag_recv.at[6 + i], **{K: 1 - k0})

    hops = [hop(0, y0, 0, up), hop(1, y0, 1, up), hop(2, y0, 1, down), hop(3, y0, 0, down)]
    for i in (0, 2, 1, 3):
        hops[i].start()
    arrive = [
        hop(0, down, 0, up), hop(1, down, 1, up), hop(2, up, 1, down),
        hop(3, up, 0, down), hop(4, far, 0, up), hop(5, far, 1, down),
    ]
    over = [across(i * 2 + h, y, h, k0) for i, y in enumerate((y0, down, up, far)) for h in range(2)]
    over[0].start()
    over[1].start()

    load_basis.wait()

    width = blocks * rhs

    def split_basis(i, acc):
        at = pl.ds(pl.multiple_of(i * CHUNK, CHUNK), CHUNK)
        for k in range(blocks):
            high, low = halves(basis[k, :, at])
            q2[pl.ds(k * rhs, rhs), at] = high
            q2[pl.ds(width + k * rhs, rhs), at] = low
        shifted = basis[blocks - 1, :, at] * diag_ref[:, at]
        w[:, at] = shifted
        stack = jnp.concatenate([q2[:, at], shifted.astype(BF16)], axis=0)
        return acc + dot(stack, q2[pl.ds(0, width), at], NT)

    made = lax.fori_loop(0, seg // CHUNK, split_basis, jnp.zeros((2 * width + rhs, width), F32))
    mine[pl.ds(0, width)] = made[:width] + made[width : 2 * width] + made[width : 2 * width].T
    mine[pl.ds(width, rhs)] = made[2 * width :]

    load = (width + rhs) // 2
    ring_axes = ((X, x0), (Z, z0), (Y, y0))
    to_pair = send(
        mine.at[pl.ds(pl.multiple_of((1 - k0) * load, 8), load)], pair, ea_send.at[0], ea_recv.at[0], **{K: 1 - k0}
    )
    to_pair.start()

    def ring_copy(i, d):
        axis, pos = ring_axes[i]
        ref = ring.at[i, pos]
        return send(ref, ref, ea_send.at[3 * i + d], ea_recv.at[3 * i + d], **{axis: lax.rem(pos + d, 4)})

    def ring_start(i, value):
        ring[i, ring_axes[i][1]] = value
        for d in range(1, 4):
            ring_copy(i, d).start()

    def ring_sum(i):
        for d in range(1, 4):
            ring_copy(i, d).wait_recv()
        return (ring[i, 0] + ring[i, 1]) + (ring[i, 2] + ring[i, 3])

    lane_slot = lax.broadcasted_iota(jnp.int32, (1, 128), 1)
    sub_slot = lax.broadcasted_iota(jnp.int32, (128, 128), 0)
    count = count_ref[0, 0]
    row_lanes, row_subs = [], []
    for c in range(slots // 128):
        row_c = rows_ref[:, pl.ds(c * 128, 128)]
        row_c = jnp.where(lane_slot + c * 128 < count, row_c, -1)
        row_lanes.append(row_c)
        row_subs.append(jnp.broadcast_to(row_c, (128, 128)).T)
    for c in range(slots // 128):
        best = jnp.zeros((1, 128), jnp.int32)
        for e in range(c + 1):
            found = row_subs[e] == row_lanes[c]
            if e == c:
                found = found & (sub_slot < lane_slot)
            best = jnp.maximum(best, jnp.max(jnp.where(found, sub_slot + (e * 128 + 1), 0), axis=0, keepdims=True))
        prev_vec[:, pl.ds(c * 128, 128)] = best
    for c in range(last_vec.shape[1] // 128):
        best = jnp.zeros((1, 128), jnp.int32)
        for e in range(slots // 128):
            found = row_subs[e] == lane_slot + c * 128
            best = jnp.maximum(best, jnp.max(jnp.where(found, sub_slot + (e * 128 + 1), 0), axis=0, keepdims=True))
        last_vec[:, pl.ds(c * 128, 128)] = best
    tables = [
        pltpu.make_async_copy(prev_vec, prev_ref, load_sem.at[6]),
        pltpu.make_async_copy(last_vec, last_ref, load_sem.at[7]),
    ]
    for copy in tables:
        copy.start()

    arrive[0].wait_recv()
    forward_up = hop(4, down, 0, up)
    forward_up.start()
    over[2].start()
    arrive[2].wait_recv()
    forward_down = hop(5, up, 1, down)
    forward_down.start()
    over[5].start()
    to_pair.wait_recv()
    ring_start(0, mine[pl.ds(pl.multiple_of(k0 * load, 8), load)] + pair[...])
    for i, j in ((1, 3), (3, 4), (4, 6), (5, 7)):
        arrive[i].wait_recv()
        over[j].start()
    ring_start(1, ring_sum(0))
    for i, y in enumerate((y0, down, up, far)):
        for h in range(2):
            across(i * 2 + h, y, h, 1 - k0).wait_recv()
    for copy in loads + tables:
        copy.wait()

    chain[0] = jnp.zeros((rhs, 128), F32)
    step = 48

    def products(i, _):
        base = i * step
        made = [dot(xg[jnp.clip(cols_ref[0, 0, base + j], 0, 8 * seg_tiles - 1)], tiles[base + j]) for j in range(step)]
        for j in range(step):
            chain[base + j + 1] = made[j] + chain[prev_ref[0, base + j]]
        return 0

    lax.fori_loop(0, slots // step, products, 0)

    ring_start(2, ring_sum(1))
    for copy in hops + over + [forward_up, forward_down]:
        copy.wait_send()

    first = ((X, x0), (Z, z0))
    second = ((Z, z0), (X, x0))

    def near(pos, d):
        return lax.rem(pos + d, 4)

    def partial(half, f, g, m):
        r = f * 4 + g if half == 0 else g * 4 + f
        return chain[last_ref[0, r * seg_tiles + half * part + m]]

    def hop1(half, i):
        axis, pos = first[half]
        return send(
            sb1.at[half, i], rb1.at[half, i], rs_send.at[half, i], rs_recv.at[half, i],
            **{axis: near(pos, 1 if i % 2 == 0 else 3)},
        )

    def hop2(half, i):
        axis, pos = second[half]
        return send(
            sb2.at[half, i], rb2.at[half, i], rs_send.at[half, 6 + i], rs_recv.at[half, 6 + i],
            **{axis: near(pos, 1 if i % 2 == 0 else 3)},
        )

    def fill1(half, i, f, h, arrived=None):
        def body(m, _):
            for g in range(2):
                value = partial(half, f, 2 * h + g, m)
                if arrived is not None:
                    value = value + rb1[half, arrived, g * part + m].astype(F32)
                sb1[half, i, g * part + m] = value.astype(BF16)
            return 0

        lax.fori_loop(0, part, body, 0, unroll=8)
        hop1(half, i).start()

    for half in range(2):
        f0 = first[half][1]
        fill1(half, 0, near(f0, 2), 0)
        fill1(half, 1, near(f0, 2), 1)
    for half in range(2):
        f0 = first[half][1]
        fill1(half, 2, near(f0, 1), 1)
        fill1(half, 3, near(f0, 3), 0)
    whole[k0] = ring_sum(2) * F32(1.0 / total_rows)
    back = send(whole.at[k0], whole.at[k0], ea_send.at[10], ea_recv.at[10], **{K: 1 - k0})
    back.start()
    for half in range(2):
        f0 = first[half][1]
        hop1(half, 0).wait_recv()
        fill1(half, 4, near(f0, 1), 0, 0)
        hop1(half, 1).wait_recv()
        fill1(half, 5, near(f0, 3), 1, 1)

    def summed1(half, g, m):
        h = g // 2
        at = (g - 2 * h) * part + m
        return (
            partial(half, first[half][1], g, m)
            + rb1[half, 3 - h, at].astype(F32)
            + rb1[half, 4 + h, at].astype(F32)
        )

    def over_part(body):
        lax.fori_loop(0, quarter, lambda m, _: (body(m), 0)[1], 0, unroll=8)

    back.wait_recv()
    products_of = jnp.concatenate([whole[0], whole[1]], axis=0)
    basis_gram = products_of[:width]
    guess = products_of[width:]
    exact = lax.Precision.HIGHEST

    def full(a, b, dims=(((1,), (0,)), ((), ()))):
        return lax.dot_general(a, b, dims, precision=exact, preferred_element_type=F32)

    guess_left = full(guess, basis_gram) - guess

    def paired(a):
        high, low = halves(a)
        top = jnp.concatenate([high, high], axis=1)
        return jnp.concatenate([top, jnp.concatenate([low, jnp.zeros_like(low)], axis=1)], axis=0)

    guess_pair = paired(guess)

    def lessen(i, _):
        at = pl.ds(pl.multiple_of(i * CHUNK, CHUNK), CHUNK)
        both = dot(guess_pair, q2[:, at])
        w[:, at] = w[:, at] - (both[:rhs] + both[rhs:])
        return 0

    lax.fori_loop(0, seg // CHUNK, lessen, 0)

    def turn(i, _):
        at = pl.ds(pl.multiple_of(i * 128, 128), 128)
        flat = jnp.concatenate([basis[k, :, at] for k in range(blocks)], axis=0).T
        high, low = halves(flat)
        qt[at, pl.ds(0, width)] = high
        qt[at, pl.ds(width, width)] = low
        return 0

    lax.fori_loop(0, seg_tiles, turn, 0, unroll=4)
    for half in range(2):
        g0 = second[half][1]
        for i in range(2, 6):
            hop1(half, i).wait_recv()

        def far_block(m):
            sb2[half, 0, m] = summed1(half, near(g0, 2), m).astype(BF16)
            sb2[half, 1, m] = summed1(half, near(g0, 2), quarter + m).astype(BF16)

        over_part(far_block)
        hop2(half, 0).start()
        hop2(half, 1).start()

        def near_block(m):
            sb2[half, 2, m] = summed1(half, near(g0, 1), quarter + m).astype(BF16)
            sb2[half, 3, m] = summed1(half, near(g0, 3), m).astype(BF16)

        over_part(near_block)
        hop2(half, 2).start()
        hop2(half, 3).start()

        def kept(m):
            zside[half, 0, m] = summed1(half, near(g0, 1), m)
            zside[half, 1, m] = summed1(half, near(g0, 3), quarter + m)
            zown[half, m] = summed1(half, g0, m)
            zown[half, quarter + m] = summed1(half, g0, quarter + m)

        over_part(kept)
    for half in range(2):
        hop2(half, 0).wait_recv()
        hop2(half, 1).wait_recv()

        def joined(m):
            sb2[half, 4, m] = (zside[half, 0, m] + rb2[half, 0, m].astype(F32)).astype(BF16)
            sb2[half, 5, m] = (zside[half, 1, m] + rb2[half, 1, m].astype(F32)).astype(BF16)

        over_part(joined)
        hop2(half, 4).start()
        hop2(half, 5).start()
    for half in range(2):
        for i in range(2, 6):
            hop2(half, i).wait_recv()

        def arrived_rows(m):
            low = lanes(half * part + m)
            w[:, low] = w[:, low] + (
                zown[half, m] + rb2[half, 3, m].astype(F32) + rb2[half, 4, m].astype(F32)
            )
            high = lanes(half * part + quarter + m)
            w[:, high] = w[:, high] + (
                zown[half, quarter + m] + rb2[half, 2, m].astype(F32) + rb2[half, 5, m].astype(F32)
            )

        over_part(arrived_rows)

    def inner_copy(d):
        p = lax.rem(c0 + d, 8)
        ref = inner.at[c0]
        return send(ref, ref, ar_send.at[d], ar_recv.at[d], **{Y: p // 2, K: lax.rem(p, 2)})

    def outer_copy(d):
        p = lax.rem(r0 + d, 16)
        ref = outer.at[r0]
        return send(ref, ref, ar_send.at[8 + d], ar_recv.at[8 + d], **{X: p // 4, Z: lax.rem(p, 4)})

    def project(i, acc):
        at = pl.ds(pl.multiple_of(i * CHUNK, CHUNK), CHUNK)
        stack = jnp.concatenate(halves(w[:, at]), axis=0)
        return acc[0] + dot(stack, qt[at, :]), acc[1] + dot(stack, stack, NT)

    with_basis, with_self = lax.fori_loop(
        0, seg // CHUNK, project, (jnp.zeros((2 * rhs, 2 * width), F32), jnp.zeros((2 * rhs, 2 * rhs), F32))
    )
    inner[c0, pl.ds(0, rhs)] = with_basis[:rhs, :width] + with_basis[rhs:, :width] + with_basis[:rhs, width:]
    with_self = with_self[:rhs, :rhs] + with_self[rhs:, :rhs] + with_self[:rhs, rhs:]
    folded = jnp.concatenate([with_self[:8], with_self[8:], jnp.zeros((8, 128 - 2 * rhs), F32)], axis=1)
    inner[c0, pl.ds(rhs, 8)] = folded
    for d in range(1, 8):
        inner_copy(d).start()
    for d in range(1, 8):
        inner_copy(d).wait_recv()
    acc = inner[0]
    for i in range(1, 8):
        acc = acc + inner[i]
    outer[r0] = acc
    for d in range(1, 16):
        outer_copy(d).start()
    for d in range(1, 16):
        outer_copy(d).wait_recv()
    acc = outer[0]
    for i in range(1, 16):
        acc = acc + outer[i]
    acc = acc * F32(1.0 / total_rows)
    reduced = acc[:rhs]
    rest = reduced + guess_left
    coef_ref[...] = (rest + guess).T
    basis_gram = jnp.concatenate([whole[0], whole[1]], axis=0)[:width]
    turned = full(rest, basis_gram) - reduced
    cross = full(turned, rest, NT) - full(rest, reduced, NT)
    gram = jnp.concatenate([acc[rhs:, :rhs], acc[rhs:, rhs : 2 * rhs]], axis=0) + cross
    gram = jnp.concatenate([gram, jnp.zeros((rhs, 128 - rhs), F32)], axis=1)

    row = lax.broadcasted_iota(jnp.int32, (rhs, 128), 0)
    lane = lax.broadcasted_iota(jnp.int32, (rhs, 128), 1)
    m = jnp.where(lane < rhs, gram, jnp.where(lane - rhs == row, F32(1), F32(0)))
    for k in range(rhs - 1):
        factor = jnp.where(row[:, :1] > k, m[:, k : k + 1] / m[k : k + 1, k : k + 1], F32(0))
        m = m - factor * m[k : k + 1, :]
    pivots = jnp.sum(jnp.where(lane == row, m, F32(0)), axis=1, keepdims=True)
    m = m / jnp.sqrt(pivots)
    tri_ref[...] = jnp.where(lane >= row, m, F32(0))[:, :rhs]
    inverse = m[:, rhs : 2 * rhs]
    back_pair = paired(-full(inverse, rest))
    inverse_pair = paired(inverse)

    def solve(i, _):
        at = pl.ds(pl.multiple_of(i * CHUNK, CHUNK), CHUNK)
        stack = jnp.concatenate(halves(w[:, at]), axis=0)
        both = dot(back_pair, q2[:, at]) + dot(inverse_pair, stack)
        out_ref[:, at] = both[:rhs] + both[rhs:]
        return 0

    lax.fori_loop(0, seg // CHUNK, solve, 0)
    for half in range(2):
        for i in range(6):
            hop1(half, i).wait_send()
            hop2(half, i).wait_send()
    for d in range(1, 8):
        inner_copy(d).wait_send()
    for d in range(1, 16):
        outer_copy(d).wait_send()
    to_pair.wait_send()
    back.wait_send()
    for i in range(3):
        for d in range(1, 4):
            ring_copy(i, d).wait_send()


def local(basis_blocks, tile_values, tile_rows, tile_column, tile_count, diagonal):
    blocks, rhs, seg = basis_blocks.shape
    slots = tile_values.shape[2]
    seg_tiles = seg // 128
    part = seg_tiles // 2
    total_rows = seg * 128
    block_tiles = seg_tiles * 16

    smem = pl.BlockSpec(memory_space=pltpu.SMEM)
    vmem = pl.BlockSpec(memory_space=pltpu.VMEM)
    hbm = pl.BlockSpec(memory_space=pl.ANY)
    dma = pltpu.SemaphoreType.DMA
    tile = (rhs, 128)
    new_block, coef, triangle = pl.pallas_call(
        functools.partial(kernel, total_rows),
        out_shape=(
            pltpu.VMEM((rhs, seg), F32),
            pltpu.VMEM((blocks * rhs, rhs), F32),
            pltpu.VMEM((rhs, rhs), F32),
        ),
        in_specs=[smem, smem, vmem, hbm, hbm, vmem],
        out_specs=(vmem, vmem, vmem),
        scratch_shapes=[
            pltpu.VMEM((blocks, rhs, seg), F32),
            pltpu.VMEM((slots, 128, 128), BF16),
            pltpu.VMEM((8 * seg_tiles, *tile), BF16),
            pltpu.VMEM((slots + 8, *tile), F32),
            pltpu.VMEM((2 * blocks * rhs, seg), BF16),
            pltpu.VMEM((seg, 2 * blocks * rhs), BF16),
            pltpu.VMEM((rhs, seg), F32),
            pltpu.VMEM((2, 6, 2 * part, *tile), BF16),
            pltpu.VMEM((2, 6, 2 * part, *tile), BF16),
            pltpu.VMEM((2, 6, part // 2, *tile), BF16),
            pltpu.VMEM((2, 6, part // 2, *tile), BF16),
            pltpu.VMEM((2, 2, part // 2, *tile), F32),
            pltpu.VMEM((2, part, *tile), F32),
            pltpu.VMEM((1, slots), jnp.int32),
            pltpu.VMEM((1, block_tiles), jnp.int32),
            pltpu.SMEM((1, slots), jnp.int32),
            pltpu.SMEM((1, block_tiles), jnp.int32),
            pltpu.VMEM((9 * rhs, 128), F32),
            pltpu.VMEM((9 * rhs // 2, 128), F32),
            pltpu.VMEM((3, 4, 9 * rhs // 2, 128), F32),
            pltpu.VMEM((2, 9 * rhs // 2, 128), F32),
            pltpu.VMEM((8, rhs + 8, 128), F32),
            pltpu.VMEM((16, rhs + 8, 128), F32),
            dma((8,)),
            dma((14,)),
            dma((14,)),
            dma((2, 12)),
            dma((2, 12)),
            dma((11,)),
            dma((11,)),
            dma((24,)),
            dma((24,)),
        ],
        compiler_params=pltpu.CompilerParams(
            collective_id=0, has_side_effects=True, vmem_limit_bytes=58 * 1024 * 1024
        ),
        name="step",
    )(tile_count, tile_column, tile_rows[0], basis_blocks, tile_values[0, 0], diagonal[None, :])
    return new_block, coef.reshape(blocks, rhs, rhs), triangle


def solution(mesh):
    split = Mesh(mesh.devices.reshape(4, 4, 4, 2), (X, Z, Y, K))
    placed = (
        P(None, None, COL_ROW),
        P(COL, ROW, None, None, None),
        P(COL, ROW, None),
        P(COL, ROW, None),
        P(COL, ROW),
        P(COL_ROW),
    )
    return jax.shard_map(
        local, mesh=split, in_specs=placed, out_specs=(P(None, COL_ROW), P(), P()), check_vma=False
    )
```

```python
import functools

import jax
import jax.numpy as jnp
from jax import lax
from jax.experimental import pallas as pl
from jax.experimental.pallas import tpu as pltpu
from jax.sharding import Mesh
from jax.sharding import PartitionSpec as P

X, Z, Y, K = "row_0", "row_1", "col_0", "col_1"
ROW = (X, Z)
COL = (Y, K)
COL_ROW = (Y, K, X, Z)
MESH = pl.DeviceIdType.MESH
F32, BF16 = jnp.float32, jnp.bfloat16
NT = (((1,), (1,)), ((), ()))
CHUNK = 1024
LONG = 4096


def send(src, dst, send_sem, recv_sem, **to):
    return pltpu.make_async_remote_copy(
        src_ref=src, dst_ref=dst, send_sem=send_sem, recv_sem=recv_sem, device_id=to, device_id_type=MESH
    )


def halves(value):
    high = value.astype(BF16)
    return high, (value - high.astype(F32)).astype(BF16)


def dot(a, b, dims=(((1,), (0,)), ((), ()))):
    return lax.dot_general(a, b, dims, preferred_element_type=F32)


def lanes(m):
    return pl.ds(pl.multiple_of(m * 128, 128), 128)


def kernel(
    total_rows,
    count_hbm, cols_hbm, rows_hbm, basis_hbm, tiles_hbm, diag_hbm,
    out_ref, coef_ref, tri_ref,
    count_ref, cols_ref, rows_ref, diag_ref,
    basis, tiles, xg0, xg1, chain, q2, qt, w,
    sb1, rb1, sb2, rb2, zside,
    prev_vec, last_vec, prev_ref, last_ref,
    mine, pair, ring, whole, inner, outer,
    load_sem, ag_send, ag_recv, rs_send, rs_recv, ea_send, ea_recv, ar_send, ar_recv,
):
    x0, z0, y0, k0 = (lax.axis_index(a) for a in (X, Z, Y, K))
    blocks, rhs, seg = basis.shape
    slots = tiles.shape[0]
    seg_tiles = seg // 128
    part = seg_tiles // 2
    quarter = part // 2
    c0 = y0 * 2 + k0
    r0 = x0 * 4 + z0

    barrier = pltpu.get_barrier_semaphore()
    inner_peers = [lax.rem(c0 + d, 8) for d in range(1, 8)]
    outer_peers = [lax.rem(r0 + d, 16) for d in range(1, 16)]
    for p in inner_peers:
        pl.semaphore_signal(barrier, inc=1, device_id={Y: p // 2, K: lax.rem(p, 2)}, device_id_type=MESH)
    for p in outer_peers:
        pl.semaphore_signal(barrier, inc=1, device_id={X: p // 4, Z: lax.rem(p, 4)}, device_id_type=MESH)

    load_vector = pltpu.make_async_copy(basis_hbm.at[blocks - 1], basis.at[blocks - 1], load_sem.at[0])
    load_basis = pltpu.make_async_copy(
        basis_hbm.at[pl.ds(0, blocks - 1)], basis.at[pl.ds(0, blocks - 1)], load_sem.at[1]
    )
    load_vector.start()
    load_basis.start()
    piece = slots // 4
    loads = [
        pltpu.make_async_copy(
            tiles_hbm.at[pl.ds(i * piece, piece)], tiles.at[pl.ds(i * piece, piece)], load_sem.at[2 + i]
        )
        for i in range(4)
    ]
    small = [
        pltpu.make_async_copy(a, b, load_sem.at[8 + i])
        for i, (a, b) in enumerate(
            ((diag_hbm, diag_ref), (rows_hbm, rows_ref), (count_hbm, count_ref), (cols_hbm, cols_ref))
        )
    ]
    for copy in small + loads:
        copy.start()

    load_vector.wait()
    own = c0 * seg_tiles

    group = rhs // 2
    xg = (xg0, xg1)

    def to_tiles(q):
        def body(m, _):
            xg[q][own + m] = basis[blocks - 1, pl.ds(q * group, group), lanes(m)].astype(BF16)
            return 0

        lax.fori_loop(0, seg_tiles, body, 0, unroll=8)

    to_tiles(0)
    pl.semaphore_wait(barrier, 22)

    up, down, far = lax.rem(y0 + 1, 4), lax.rem(y0 + 3, 4), lax.rem(y0 + 2, 4)

    def chunk(q, y, k, h):
        return xg[q].at[pl.ds((y * 2 + k) * seg_tiles + h * part, part)]

    def hop(q, i, y, h, to):
        ref = chunk(q, y, k0, h)
        return send(ref, ref, ag_send.at[q, 0], ag_recv.at[q, i], **{Y: to})

    def across(q, y, h, k):
        ref = chunk(q, y, k, h)
        return send(ref, ref, ag_send.at[q, 1], ag_recv.at[q, 6], **{K: 1 - k0})

    hops = [
        [hop(q, 0, y0, 0, up), hop(q, 1, y0, 1, up), hop(q, 2, y0, 1, down), hop(q, 3, y0, 0, down)]
        for q in range(2)
    ]
    arrive = [
        [
            hop(q, 0, down, 0, up), hop(q, 1, down, 1, up), hop(q, 2, up, 1, down),
            hop(q, 3, up, 0, down), hop(q, 4, far, 0, up), hop(q, 5, far, 1, down),
        ]
        for q in range(2)
    ]
    forward = [[hop(q, 4, down, 0, up), hop(q, 5, up, 1, down)] for q in range(2)]
    places = list(enumerate((y0, down, up, far)))
    over = [[across(q, y, h, k0) for i, y in places for h in range(2)] for q in range(2)]

    def crossed(q):
        ref = xg[q].at[pl.ds(0, 4 * seg_tiles)]
        send(ref, ref, ag_send.at[q, 1], ag_recv.at[q, 6], **{K: 1 - k0}).wait_recv()

    def depart(q):
        for i in (0, 2, 1, 3):
            hops[q][i].start()
        over[q][0].start()
        over[q][1].start()

    def pass_on(q):
        for i, j, f in ((0, 2, 0), (2, 5, 1)):
            arrive[q][i].wait_recv()
            forward[q][f].start()
            over[q][j].start()

    def take(q, pairs):
        for i, j in pairs:
            arrive[q][i].wait_recv()
            over[q][j].start()

    depart(0)
    to_tiles(1)

    load_basis.wait()
    for copy in small:
        copy.wait()

    width = blocks * rhs

    def split_basis(i, acc):
        at = pl.ds(pl.multiple_of(i * CHUNK, CHUNK), CHUNK)
        for k in range(blocks):
            high, low = halves(basis[k, :, at])
            q2[pl.ds(k * rhs, rhs), at] = high
            q2[pl.ds(width + k * rhs, rhs), at] = low
        shifted = basis[blocks - 1, :, at] * diag_ref[:, at]
        w[:, at] = shifted
        stack = jnp.concatenate([q2[:, at], shifted.astype(BF16)], axis=0)
        return acc + dot(stack, q2[pl.ds(0, width), at], NT)

    made = lax.fori_loop(0, seg // CHUNK, split_basis, jnp.zeros((2 * width + rhs, width), F32))
    mine[pl.ds(0, width)] = made[:width] + made[width : 2 * width] + made[width : 2 * width].T
    mine[pl.ds(width, rhs)] = made[2 * width :]

    load = (width + rhs) // 2
    ring_axes = ((X, x0), (Z, z0), (Y, y0))
    to_pair = send(
        mine.at[pl.ds(pl.multiple_of((1 - k0) * load, 8), load)], pair, ea_send.at[0], ea_recv.at[0], **{K: 1 - k0}
    )
    to_pair.start()

    def ring_copy(i, d):
        axis, pos = ring_axes[i]
        ref = ring.at[i, pos]
        return send(ref, ref, ea_send.at[1], ea_recv.at[1 + i], **{axis: lax.rem(pos + d, 4)})

    def ring_start(i, value):
        ring[i, ring_axes[i][1]] = value
        for d in range(1, 4):
            ring_copy(i, d).start()

    def ring_sum(i):
        ref = ring.at[i, pl.ds(0, 3)]
        send(ref, ref, ea_send.at[1], ea_recv.at[1 + i], **{ring_axes[i][0]: 0}).wait_recv()
        return (ring[i, 0] + ring[i, 1]) + (ring[i, 2] + ring[i, 3])

    lane_slot = lax.broadcasted_iota(jnp.int32, (1, 128), 1)
    sub_slot = lax.broadcasted_iota(jnp.int32, (128, 128), 0)
    count = count_ref[...]
    row_lanes, row_subs = [], []
    for c in range(slots // 128):
        row_c = rows_ref[:, pl.ds(c * 128, 128)]
        row_c = jnp.where(lane_slot + c * 128 < count, row_c, -1)
        row_lanes.append(row_c)
        row_subs.append(jnp.broadcast_to(row_c, (128, 128)).T)
    for c in range(slots // 128):
        best = jnp.zeros((1, 128), jnp.int32)
        for e in range(c + 1):
            found = row_subs[e] == row_lanes[c]
            if e == c:
                found = found & (sub_slot < lane_slot)
            best = jnp.maximum(best, jnp.max(jnp.where(found, sub_slot + (e * 128 + 1), 0), axis=0, keepdims=True))
        prev_vec[:, pl.ds(c * 128, 128)] = best
    for c in range(last_vec.shape[1] // 128):
        best = jnp.zeros((1, 128), jnp.int32)
        for e in range(slots // 128):
            found = row_subs[e] == lane_slot + c * 128
            best = jnp.maximum(best, jnp.max(jnp.where(found, sub_slot + (e * 128 + 1), 0), axis=0, keepdims=True))
        last_vec[:, pl.ds(c * 128, 128)] = best
    tables = [
        pltpu.make_async_copy(prev_vec, prev_ref, load_sem.at[6]),
        pltpu.make_async_copy(last_vec, last_ref, load_sem.at[7]),
    ]
    for copy in tables:
        copy.start()

    pass_on(0)
    depart(1)
    to_pair.wait_recv()
    ring_start(0, mine[pl.ds(pl.multiple_of(k0 * load, 8), load)] + pair[...])
    take(0, ((1, 3), (3, 4), (4, 6), (5, 7)))
    crossed(0)
    for copy in loads + tables:
        copy.wait()

    step = 48
    trips = slots // step

    def products(q, start, stop):

        def body(i, _):
            base = i * step
            made = [
                dot(xg[q][jnp.clip(cols_ref[0, 0, base + j], 0, 8 * seg_tiles - 1)], tiles[base + j])
                for j in range(step)
            ]
            for j in range(step):
                chain[q, base + j + 1] = made[j] + chain[q, prev_ref[0, base + j]]
            return 0

        lax.fori_loop(start, stop, body, 0)

    chain[0, 0] = jnp.zeros((group, 128), F32)
    chain[1, 0] = jnp.zeros((group, 128), F32)
    products(0, 0, trips // 4)
    pass_on(1)
    take(1, ((1, 3), (3, 4)))
    products(0, trips // 4, trips // 2)
    ring_start(1, ring_sum(0))
    products(0, trips // 2, trips)
    take(1, ((4, 6), (5, 7)))

    first = ((X, x0), (Z, z0))
    second = ((Z, z0), (X, x0))

    def near(pos, d):
        return lax.rem(pos + d, 4)

    def partial(q, half, f, g, p):
        r = f * 4 + g if half == 0 else g * 4 + f
        at = r * seg_tiles + half * part + 2 * p
        return jnp.concatenate([chain[q, last_ref[0, at]], chain[q, last_ref[0, at + 1]]], axis=0)

    ahead = (2, 1, 3, 0)
    eighth = quarter // 2
    onward, stay = (0, 1, 2), (3,)

    def hop1(q, half, i, os):
        axis, pos = first[half]
        n = 2 * q + half
        at = pl.ds(os[0] * eighth, len(os) * eighth)
        return send(
            sb1.at[n, i, at], rb1.at[n, i, at], rs_send.at[0], rs_recv.at[n, min(i, 2) + (3 if os == stay else 0)],
            **{axis: near(pos, 1 if i % 2 == 0 else 3)},
        )

    def hop2(q, half, i):
        axis, pos = second[half]
        n = 2 * q + half
        return send(
            sb2.at[n, i], rb2.at[n, i], rs_send.at[1], rs_recv.at[n, 6 + min(i, 2)],
            **{axis: near(pos, 1 if i % 2 == 0 else 3)},
        )

    def own_block(q, half, f, o, p):
        return partial(q, half, f, near(second[half][1], ahead[o]), p)

    def fill1(q, half, i, f, h, os, arrived=None):
        n = 2 * q + half

        def body(p, _):
            for o in os:
                value = own_block(q, half, f, o, h * eighth + p)
                if arrived is not None:
                    value = value + rb1[n, arrived, o * eighth + p].astype(F32)
                sb1[n, i, o * eighth + p] = value.astype(BF16)
            return 0

        lax.fori_loop(0, eighth, body, 0, unroll=8)
        hop1(q, half, i, os).start()

    def phase1(q, os):
        for half in range(2):
            f0 = first[half][1]
            fill1(q, half, 0, near(f0, 2), 0, os)
            fill1(q, half, 1, near(f0, 2), 1, os)
        for half in range(2):
            f0 = first[half][1]
            fill1(q, half, 2, near(f0, 1), 1, os)
            fill1(q, half, 3, near(f0, 3), 0, os)

    def phase1_rest(q, os):
        for half in range(2):
            f0 = first[half][1]
            hop1(q, half, 0, os).wait_recv()
            fill1(q, half, 4, near(f0, 1), 0, os, 0)
            hop1(q, half, 1, os).wait_recv()
            fill1(q, half, 5, near(f0, 3), 1, os, 1)

    def wait_rest1(q, half, os):
        n = 2 * q + half
        ref = rb1.at[n, pl.ds(2, 4), pl.ds(os[0] * eighth, len(os) * eighth)]
        send(ref, ref, rs_send.at[0], rs_recv.at[n, 2 + (3 if os == stay else 0)], **{X: 0}).wait_recv()

    def wait_rest2(q, half):
        n = 2 * q + half
        ref = rb2.at[n, pl.ds(2, 4)]
        send(ref, ref, rs_send.at[1], rs_recv.at[n, 8], **{X: 0}).wait_recv()

    def summed1(q, half, o, h, p):
        n = 2 * q + half
        return (
            own_block(q, half, first[half][1], o, h * eighth + p)
            + rb1[n, 3 - h, o * eighth + p].astype(F32)
            + rb1[n, 4 + h, o * eighth + p].astype(F32)
        )

    def over_part(body):
        lax.fori_loop(0, eighth, lambda p, _: (body(p), 0)[1], 0, unroll=8)

    def phase2(q):
        for half in range(2):
            n = 2 * q + half
            wait_rest1(q, half, onward)

            def far_block(p):
                sb2[n, 0, p] = summed1(q, half, 0, 0, p).astype(BF16)
                sb2[n, 1, p] = summed1(q, half, 0, 1, p).astype(BF16)

            over_part(far_block)
            hop2(q, half, 0).start()
            hop2(q, half, 1).start()
        for half in range(2):
            n = 2 * q + half

            def near_block(p):
                sb2[n, 2, p] = summed1(q, half, 1, 1, p).astype(BF16)
                sb2[n, 3, p] = summed1(q, half, 2, 0, p).astype(BF16)

            over_part(near_block)
            hop2(q, half, 2).start()
            hop2(q, half, 3).start()
        for half in range(2):
            n = 2 * q + half

            def kept(p):
                zside[n, 0, p] = summed1(q, half, 1, 0, p)
                zside[n, 1, p] = summed1(q, half, 2, 1, p)

            over_part(kept)

    def phase2_rest(q):
        for half in range(2):
            n = 2 * q + half
            hop2(q, half, 0).wait_recv()
            hop2(q, half, 1).wait_recv()

            def joined(p):
                sb2[n, 4, p] = (zside[n, 0, p] + rb2[n, 0, p].astype(F32)).astype(BF16)
                sb2[n, 5, p] = (zside[n, 1, p] + rb2[n, 1, p].astype(F32)).astype(BF16)

            over_part(joined)
            hop2(q, half, 4).start()
            hop2(q, half, 5).start()

    def place(q, half, m, value):
        for e in range(2):
            at = (pl.ds(q * group, group), lanes(half * part + m + e))
            w[at] = w[at] + value[e * group : (e + 1) * group]

    def stayed(q):
        for half in range(2):
            wait_rest1(q, half, stay)

            def body(p):
                place(q, half, 2 * p, summed1(q, half, 3, 0, p))
                place(q, half, quarter + 2 * p, summed1(q, half, 3, 1, p))

            over_part(body)

    def landed(q):
        for half in range(2):
            n = 2 * q + half
            wait_rest2(q, half)

            def body(p):
                place(q, half, 2 * p, rb2[n, 3, p].astype(F32) + rb2[n, 4, p].astype(F32))
                place(q, half, quarter + 2 * p, rb2[n, 2, p].astype(F32) + rb2[n, 5, p].astype(F32))

            over_part(body)

    phase1(0, onward)
    phase1(0, stay)
    crossed(1)
    products(1, 0, trips // 2)
    ring_start(2, ring_sum(1))
    products(1, trips // 2, trips)
    phase1_rest(0, onward)
    phase1(1, onward)
    phase1_rest(0, stay)
    phase1(1, stay)
    whole[k0] = ring_sum(2) * F32(1.0 / total_rows)
    back = send(whole.at[k0], whole.at[k0], ea_send.at[2], ea_recv.at[4], **{K: 1 - k0})
    back.start()
    for q in range(2):
        ref = xg[q].at[pl.ds(0, 3 * seg_tiles)]
        send(ref, ref, ag_send.at[q, 0], ag_recv.at[q, 0], **{Y: up}).wait_send()
        ref = xg[q].at[pl.ds(0, 4 * seg_tiles)]
        send(ref, ref, ag_send.at[q, 1], ag_recv.at[q, 6], **{K: 1 - k0}).wait_send()
    back.wait_recv()
    products_of = jnp.concatenate([whole[0], whole[1]], axis=0)
    basis_gram = products_of[:width]
    guess = products_of[width:]
    exact = lax.Precision.HIGHEST

    def full(a, b, dims=(((1,), (0,)), ((), ()))):
        return lax.dot_general(a, b, dims, precision=exact, preferred_element_type=F32)

    guess_left = full(guess, basis_gram) - guess

    def paired(a):
        high, low = halves(a)
        top = jnp.concatenate([high, high], axis=1)
        return jnp.concatenate([top, jnp.concatenate([low, jnp.zeros_like(low)], axis=1)], axis=0)

    guess_pair = paired(guess)

    def lessen(i, _):
        at = pl.ds(pl.multiple_of(i * CHUNK, CHUNK), CHUNK)
        both = dot(guess_pair, q2[:, at])
        w[:, at] = w[:, at] - (both[:rhs] + both[rhs:])
        return 0

    lax.fori_loop(0, seg // CHUNK, lessen, 0)
    phase2(0)

    def turn(i, _):
        at = pl.ds(pl.multiple_of(i * 128, 128), 128)
        flat = jnp.concatenate([basis[k, :, at] for k in range(blocks)], axis=0).T
        high, low = halves(flat)
        qt[at, pl.ds(0, width)] = high
        qt[at, pl.ds(width, width)] = low
        return 0

    lax.fori_loop(0, seg_tiles, turn, 0, unroll=4)
    phase1_rest(1, onward)
    phase2(1)
    phase2_rest(0)
    phase1_rest(1, stay)
    stayed(0)
    phase2_rest(1)
    landed(0)
    stayed(1)
    landed(1)

    def inner_copy(d):
        p = lax.rem(c0 + d, 8)
        ref = inner.at[c0]
        return send(ref, ref, ar_send.at[0], ar_recv.at[0], **{Y: p // 2, K: lax.rem(p, 2)})

    def outer_copy(d):
        p = lax.rem(r0 + d, 16)
        ref = outer.at[r0]
        return send(ref, ref, ar_send.at[1], ar_recv.at[1], **{X: p // 4, Z: lax.rem(p, 4)})

    def inner_all():
        ref = inner.at[pl.ds(0, 7)]
        return send(ref, ref, ar_send.at[0], ar_recv.at[0], **{Y: 0})

    def outer_all():
        ref = outer.at[pl.ds(0, 15)]
        return send(ref, ref, ar_send.at[1], ar_recv.at[1], **{X: 0})

    def project(i, acc):
        at = pl.ds(pl.multiple_of(i * LONG, LONG), LONG)
        stack = jnp.concatenate(halves(w[:, at]), axis=0)
        return acc[0] + dot(stack, qt[at, :]), acc[1] + dot(stack, stack, NT)

    with_basis, with_self = lax.fori_loop(
        0, seg // LONG, project, (jnp.zeros((2 * rhs, 2 * width), F32), jnp.zeros((2 * rhs, 2 * rhs), F32))
    )
    inner[c0, pl.ds(0, rhs)] = with_basis[:rhs, :width] + with_basis[rhs:, :width] + with_basis[:rhs, width:]
    with_self = with_self[:rhs, :rhs] + with_self[rhs:, :rhs] + with_self[:rhs, rhs:]
    folded = jnp.concatenate([with_self[:8], with_self[8:], jnp.zeros((8, 128 - 2 * rhs), F32)], axis=1)
    inner[c0, pl.ds(rhs, 8)] = folded
    for d in range(1, 8):
        inner_copy(d).start()
    inner_all().wait_recv()
    acc = inner[0]
    for i in range(1, 8):
        acc = acc + inner[i]
    outer[r0] = acc
    for d in range(1, 16):
        outer_copy(d).start()
    outer_all().wait_recv()
    acc = outer[0]
    for i in range(1, 16):
        acc = acc + outer[i]
    acc = acc * F32(1.0 / total_rows)
    reduced = acc[:rhs]
    rest = reduced + guess_left
    coef_ref[...] = (rest + guess).T
    basis_gram = jnp.concatenate([whole[0], whole[1]], axis=0)[:width]
    turned = full(rest, basis_gram) - reduced
    cross = full(turned, rest, NT) - full(rest, reduced, NT)
    gram = jnp.concatenate([acc[rhs:, :rhs], acc[rhs:, rhs : 2 * rhs]], axis=0) + cross
    gram = jnp.concatenate([gram, jnp.zeros((rhs, 128 - rhs), F32)], axis=1)

    row = lax.broadcasted_iota(jnp.int32, (rhs, 128), 0)
    lane = lax.broadcasted_iota(jnp.int32, (rhs, 128), 1)
    m = jnp.where(lane < rhs, gram, jnp.where(lane - rhs == row, F32(1), F32(0)))
    for k in range(rhs - 1):
        column = jnp.broadcast_to(m[:, k : k + 1], m.shape)
        m = m - jnp.where(row > k, column * (1.0 / column[k : k + 1, :]), F32(0)) * m[k : k + 1, :]
    pivots = jnp.sum(jnp.where(lane == row, m, F32(0)), axis=1, keepdims=True)
    m = m / jnp.sqrt(pivots)
    tri_ref[...] = jnp.where(lane >= row, m, F32(0))[:, :rhs]
    inverse = m[:, rhs : 2 * rhs]
    back_pair = paired(-full(inverse, rest))
    inverse_pair = paired(inverse)

    def solve(i, _):
        at = pl.ds(pl.multiple_of(i * LONG, LONG), LONG)
        stack = jnp.concatenate(halves(w[:, at]), axis=0)
        both = dot(back_pair, q2[:, at]) + dot(inverse_pair, stack)
        out_ref[:, at] = both[:rhs] + both[rhs:]
        return 0

    lax.fori_loop(0, seg // LONG, solve, 0)
    send(sb1, sb1, rs_send.at[0], rs_recv.at[0, 0], **{X: 0}).wait_send()
    send(sb2, sb2, rs_send.at[1], rs_recv.at[0, 0], **{X: 0}).wait_send()
    inner_all().wait_send()
    outer_all().wait_send()
    to_pair.wait_send()
    back.wait_send()
    ref = ring.at[:, pl.ds(0, 3)]
    send(ref, ref, ea_send.at[1], ea_recv.at[1], **{X: 0}).wait_send()


def local(basis_blocks, tile_values, tile_rows, tile_column, tile_count, diagonal):
    blocks, rhs, seg = basis_blocks.shape
    slots = tile_values.shape[2]
    seg_tiles = seg // 128
    part = seg_tiles // 2
    total_rows = seg * 128
    block_tiles = seg_tiles * 16

    vmem = pl.BlockSpec(memory_space=pltpu.VMEM)
    hbm = pl.BlockSpec(memory_space=pl.ANY)
    dma = pltpu.SemaphoreType.DMA
    tile = (rhs, 128)
    new_block, coef, triangle = pl.pallas_call(
        functools.partial(kernel, total_rows),
        out_shape=(
            pltpu.VMEM((rhs, seg), F32),
            pltpu.VMEM((blocks * rhs, rhs), F32),
            pltpu.VMEM((rhs, rhs), F32),
        ),
        in_specs=[hbm] * 6,
        out_specs=(vmem, vmem, vmem),
        scratch_shapes=[
            pltpu.VMEM((1, 1), jnp.int32),
            pltpu.SMEM((1, 1, slots), jnp.int32),
            pltpu.VMEM((1, slots), jnp.int32),
            pltpu.VMEM((1, seg), F32),
            pltpu.VMEM((blocks, rhs, seg), F32),
            pltpu.VMEM((slots, 128, 128), BF16),
            pltpu.VMEM((8 * seg_tiles, rhs // 2, 128), BF16),
            pltpu.VMEM((8 * seg_tiles, rhs // 2, 128), BF16),
            pltpu.VMEM((2, slots + 8, rhs // 2, 128), F32),
            pltpu.VMEM((2 * blocks * rhs, seg), BF16),
            pltpu.VMEM((seg, 2 * blocks * rhs), BF16),
            pltpu.VMEM((rhs, seg), F32),
            pltpu.VMEM((4, 6, part, *tile), BF16),
            pltpu.VMEM((4, 6, part, *tile), BF16),
            pltpu.VMEM((4, 6, part // 4, *tile), BF16),
            pltpu.VMEM((4, 6, part // 4, *tile), BF16),
            pltpu.VMEM((4, 2, part // 4, *tile), F32),
            pltpu.VMEM((1, slots), jnp.int32),
            pltpu.VMEM((1, block_tiles), jnp.int32),
            pltpu.SMEM((1, slots), jnp.int32),
            pltpu.SMEM((1, block_tiles), jnp.int32),
            pltpu.VMEM((9 * rhs, 128), F32),
            pltpu.VMEM((9 * rhs // 2, 128), F32),
            pltpu.VMEM((3, 4, 9 * rhs // 2, 128), F32),
            pltpu.VMEM((2, 9 * rhs // 2, 128), F32),
            pltpu.VMEM((8, rhs + 8, 128), F32),
            pltpu.VMEM((16, rhs + 8, 128), F32),
            dma((12,)),
            dma((2, 2)),
            dma((2, 7)),
            dma((2,)),
            dma((4, 9)),
            dma((3,)),
            dma((5,)),
            dma((2,)),
            dma((2,)),
        ],
        compiler_params=pltpu.CompilerParams(
            collective_id=0, has_side_effects=True, vmem_limit_bytes=58 * 1024 * 1024
        ),
        name="step",
    )(tile_count, tile_column, tile_rows[0], basis_blocks, tile_values[0, 0], diagonal[None, :])
    return new_block, coef.reshape(blocks, rhs, rhs), triangle


def solution(mesh):
    split = Mesh(mesh.devices.reshape(4, 4, 4, 2), (X, Z, Y, K))
    placed = (
        P(None, None, COL_ROW),
        P(COL, ROW, None, None, None),
        P(COL, ROW, None),
        P(COL, ROW, None),
        P(COL, ROW),
        P(COL_ROW),
    )
    return jax.shard_map(
        local, mesh=split, in_specs=placed, out_specs=(P(None, COL_ROW), P(), P()), check_vma=False
    )
```

```python
import functools

import jax
import jax.numpy as jnp
from jax import lax
from jax.experimental import pallas as pl
from jax.experimental.pallas import tpu as pltpu
from jax.sharding import Mesh
from jax.sharding import PartitionSpec as P

X, Z, Y, K = "row_0", "row_1", "col_0", "col_1"
ROW = (X, Z)
COL = (Y, K)
COL_ROW = (Y, K, X, Z)
MESH = pl.DeviceIdType.MESH
F32, BF16 = jnp.float32, jnp.bfloat16
NT = (((1,), (1,)), ((), ()))
CHUNK = 1024
LONG = 4096
FINISH = 2048


def send(src, dst, send_sem, recv_sem, **to):
    return pltpu.make_async_remote_copy(
        src_ref=src, dst_ref=dst, send_sem=send_sem, recv_sem=recv_sem, device_id=to, device_id_type=MESH
    )


def halves(value):
    high = value.astype(BF16)
    return high, (value - high.astype(F32)).astype(BF16)


def dot(a, b, dims=(((1,), (0,)), ((), ()))):
    return lax.dot_general(a, b, dims, preferred_element_type=F32)


def lanes(m):
    return pl.ds(pl.multiple_of(m * 128, 128), 128)


def kernel(
    total_rows,
    count_hbm, cols_hbm, rows_hbm, basis_hbm, tiles_hbm, diag_hbm,
    w, q2, pairs_ref, coef_ref, tri_ref,
    count_ref, cols_ref, rows_ref, diag_ref,
    basis, tiles, xg0, xg1, chain, qt,
    sb1, rb1, sb2, rb2, zside,
    prev_vec, last_vec, prev_ref, last_ref,
    mine, pair, ring, whole, inner, outer,
    load_sem, ag_send, ag_recv, rs_send, rs_recv, ea_send, ea_recv, ar_send, ar_recv,
):
    x0, z0, y0, k0 = (lax.axis_index(a) for a in (X, Z, Y, K))
    blocks, rhs, seg = basis.shape
    slots = tiles.shape[0]
    seg_tiles = seg // 128
    part = seg_tiles // 2
    quarter = part // 2
    c0 = y0 * 2 + k0
    r0 = x0 * 4 + z0

    barrier = pltpu.get_barrier_semaphore()
    inner_peers = [lax.rem(c0 + d, 8) for d in range(1, 8)]
    outer_peers = [lax.rem(r0 + d, 16) for d in range(1, 16)]
    for p in inner_peers:
        pl.semaphore_signal(barrier, inc=1, device_id={Y: p // 2, K: lax.rem(p, 2)}, device_id_type=MESH)
    for p in outer_peers:
        pl.semaphore_signal(barrier, inc=1, device_id={X: p // 4, Z: lax.rem(p, 4)}, device_id_type=MESH)

    load_vector = pltpu.make_async_copy(basis_hbm.at[blocks - 1], basis.at[blocks - 1], load_sem.at[0])
    load_basis = pltpu.make_async_copy(
        basis_hbm.at[pl.ds(0, blocks - 1)], basis.at[pl.ds(0, blocks - 1)], load_sem.at[1]
    )
    load_vector.start()
    load_basis.start()
    piece = slots // 4
    loads = [
        pltpu.make_async_copy(
            tiles_hbm.at[pl.ds(i * piece, piece)], tiles.at[pl.ds(i * piece, piece)], load_sem.at[2 + i]
        )
        for i in range(4)
    ]
    small = [
        pltpu.make_async_copy(a, b, load_sem.at[8 + i])
        for i, (a, b) in enumerate(
            ((diag_hbm, diag_ref), (rows_hbm, rows_ref), (count_hbm, count_ref), (cols_hbm, cols_ref))
        )
    ]
    for copy in small + loads:
        copy.start()

    load_vector.wait()
    own = c0 * seg_tiles

    group = rhs // 2
    xg = (xg0, xg1)

    def to_tiles(q):
        def body(m, _):
            xg[q][own + m] = basis[blocks - 1, pl.ds(q * group, group), lanes(m)].astype(BF16)
            return 0

        lax.fori_loop(0, seg_tiles, body, 0, unroll=8)

    to_tiles(0)
    pl.semaphore_wait(barrier, 22)

    up, down, far = lax.rem(y0 + 1, 4), lax.rem(y0 + 3, 4), lax.rem(y0 + 2, 4)

    def chunk(q, y, k, h):
        return xg[q].at[pl.ds((y * 2 + k) * seg_tiles + h * part, part)]

    def hop(q, i, y, h, to):
        ref = chunk(q, y, k0, h)
        return send(ref, ref, ag_send.at[q, 0], ag_recv.at[q, i], **{Y: to})

    def across(q, y, h, k):
        ref = chunk(q, y, k, h)
        return send(ref, ref, ag_send.at[q, 1], ag_recv.at[q, 6], **{K: 1 - k0})

    hops = [
        [hop(q, 0, y0, 0, up), hop(q, 1, y0, 1, up), hop(q, 2, y0, 1, down), hop(q, 3, y0, 0, down)]
        for q in range(2)
    ]
    arrive = [
        [
            hop(q, 0, down, 0, up), hop(q, 1, down, 1, up), hop(q, 2, up, 1, down),
            hop(q, 3, up, 0, down), hop(q, 4, far, 0, up), hop(q, 5, far, 1, down),
        ]
        for q in range(2)
    ]
    forward = [[hop(q, 4, down, 0, up), hop(q, 5, up, 1, down)] for q in range(2)]
    places = list(enumerate((y0, down, up, far)))
    over = [[across(q, y, h, k0) for i, y in places for h in range(2)] for q in range(2)]

    def crossed(q):
        ref = xg[q].at[pl.ds(0, 4 * seg_tiles)]
        send(ref, ref, ag_send.at[q, 1], ag_recv.at[q, 6], **{K: 1 - k0}).wait_recv()

    def depart(q):
        for i in (0, 2, 1, 3):
            hops[q][i].start()
        over[q][0].start()
        over[q][1].start()

    def pass_on(q):
        for i, j, f in ((0, 2, 0), (2, 5, 1)):
            arrive[q][i].wait_recv()
            forward[q][f].start()
            over[q][j].start()

    def take(q, pairs):
        for i, j in pairs:
            arrive[q][i].wait_recv()
            over[q][j].start()

    depart(0)
    to_tiles(1)

    load_basis.wait()
    for copy in small:
        copy.wait()

    width = blocks * rhs

    def split_basis(i, acc):
        at = pl.ds(pl.multiple_of(i * CHUNK, CHUNK), CHUNK)
        for k in range(blocks):
            high, low = halves(basis[k, :, at])
            q2[pl.ds(k * rhs, rhs), at] = high
            q2[pl.ds(width + k * rhs, rhs), at] = low
        shifted = basis[blocks - 1, :, at] * diag_ref[:, at]
        w[:, at] = shifted
        stack = jnp.concatenate([q2[:, at], shifted.astype(BF16)], axis=0)
        return acc + dot(stack, q2[pl.ds(0, width), at], NT)

    made = lax.fori_loop(0, seg // CHUNK, split_basis, jnp.zeros((2 * width + rhs, width), F32))
    mine[pl.ds(0, width)] = made[:width] + made[width : 2 * width] + made[width : 2 * width].T
    mine[pl.ds(width, rhs)] = made[2 * width :]

    load = (width + rhs) // 2
    ring_axes = ((X, x0), (Z, z0), (Y, y0))
    to_pair = send(
        mine.at[pl.ds(pl.multiple_of((1 - k0) * load, 8), load)], pair, ea_send.at[0], ea_recv.at[0], **{K: 1 - k0}
    )
    to_pair.start()

    def ring_copy(i, d):
        axis, pos = ring_axes[i]
        ref = ring.at[i, pos]
        return send(ref, ref, ea_send.at[1], ea_recv.at[1 + i], **{axis: lax.rem(pos + d, 4)})

    def ring_start(i, value):
        ring[i, ring_axes[i][1]] = value
        for d in range(1, 4):
            ring_copy(i, d).start()

    def ring_sum(i):
        ref = ring.at[i, pl.ds(0, 3)]
        send(ref, ref, ea_send.at[1], ea_recv.at[1 + i], **{ring_axes[i][0]: 0}).wait_recv()
        return (ring[i, 0] + ring[i, 1]) + (ring[i, 2] + ring[i, 3])

    lane_slot = lax.broadcasted_iota(jnp.int32, (1, 128), 1)
    sub_slot = lax.broadcasted_iota(jnp.int32, (128, 128), 0)
    count = count_ref[...]
    row_lanes, row_subs = [], []
    for c in range(slots // 128):
        row_c = rows_ref[:, pl.ds(c * 128, 128)]
        row_c = jnp.where(lane_slot + c * 128 < count, row_c, -1)
        row_lanes.append(row_c)
        row_subs.append(jnp.broadcast_to(row_c, (128, 128)).T)
    for c in range(slots // 128):
        best = jnp.zeros((1, 128), jnp.int32)
        for e in range(c + 1):
            found = row_subs[e] == row_lanes[c]
            if e == c:
                found = found & (sub_slot < lane_slot)
            best = jnp.maximum(best, jnp.max(jnp.where(found, sub_slot + (e * 128 + 1), 0), axis=0, keepdims=True))
        prev_vec[:, pl.ds(c * 128, 128)] = best
    for c in range(last_vec.shape[1] // 128):
        best = jnp.zeros((1, 128), jnp.int32)
        for e in range(slots // 128):
            found = row_subs[e] == lane_slot + c * 128
            best = jnp.maximum(best, jnp.max(jnp.where(found, sub_slot + (e * 128 + 1), 0), axis=0, keepdims=True))
        last_vec[:, pl.ds(c * 128, 128)] = best
    tables = [
        pltpu.make_async_copy(prev_vec, prev_ref, load_sem.at[6]),
        pltpu.make_async_copy(last_vec, last_ref, load_sem.at[7]),
    ]
    for copy in tables:
        copy.start()

    pass_on(0)
    depart(1)
    to_pair.wait_recv()
    ring_start(0, mine[pl.ds(pl.multiple_of(k0 * load, 8), load)] + pair[...])
    take(0, ((1, 3), (3, 4), (4, 6), (5, 7)))
    crossed(0)
    for copy in loads + tables:
        copy.wait()

    step = 48
    trips = slots // step

    def products(q, start, stop):

        def body(i, _):
            base = i * step
            made = [
                dot(xg[q][jnp.clip(cols_ref[0, 0, base + j], 0, 8 * seg_tiles - 1)], tiles[base + j])
                for j in range(step)
            ]
            for j in range(step):
                chain[q, base + j + 1] = made[j] + chain[q, prev_ref[0, base + j]]
            return 0

        lax.fori_loop(start, stop, body, 0)

    chain[0, 0] = jnp.zeros((group, 128), F32)
    chain[1, 0] = jnp.zeros((group, 128), F32)
    products(0, 0, trips // 4)
    pass_on(1)
    take(1, ((1, 3), (3, 4)))
    products(0, trips // 4, trips // 2)
    ring_start(1, ring_sum(0))
    products(0, trips // 2, trips)
    take(1, ((4, 6), (5, 7)))

    first = ((X, x0), (Z, z0))
    second = ((Z, z0), (X, x0))

    def near(pos, d):
        return lax.rem(pos + d, 4)

    def partial(q, half, f, g, p):
        r = f * 4 + g if half == 0 else g * 4 + f
        at = r * seg_tiles + half * part + 2 * p
        return jnp.concatenate([chain[q, last_ref[0, at]], chain[q, last_ref[0, at + 1]]], axis=0)

    ahead = (2, 1, 3, 0)
    eighth = quarter // 2
    onward, stay = (0, 1, 2), (3,)

    def hop1(q, half, i, os):
        axis, pos = first[half]
        n = 2 * q + half
        at = pl.ds(os[0] * eighth, len(os) * eighth)
        return send(
            sb1.at[n, i, at], rb1.at[n, i, at], rs_send.at[0], rs_recv.at[n, min(i, 2) + (3 if os == stay else 0)],
            **{axis: near(pos, 1 if i % 2 == 0 else 3)},
        )

    def hop2(q, half, i):
        axis, pos = second[half]
        n = 2 * q + half
        return send(
            sb2.at[n, i], rb2.at[n, i], rs_send.at[1], rs_recv.at[n, 6 + min(i, 2)],
            **{axis: near(pos, 1 if i % 2 == 0 else 3)},
        )

    def own_block(q, half, f, o, p):
        return partial(q, half, f, near(second[half][1], ahead[o]), p)

    def fill1(q, half, i, f, h, os, arrived=None):
        n = 2 * q + half

        def body(p, _):
            for o in os:
                value = own_block(q, half, f, o, h * eighth + p)
                if arrived is not None:
                    value = value + rb1[n, arrived, o * eighth + p].astype(F32)
                sb1[n, i, o * eighth + p] = value.astype(BF16)
            return 0

        lax.fori_loop(0, eighth, body, 0, unroll=8)
        hop1(q, half, i, os).start()

    def phase1(q, os):
        for half in range(2):
            f0 = first[half][1]
            fill1(q, half, 0, near(f0, 2), 0, os)
            fill1(q, half, 1, near(f0, 2), 1, os)
        for half in range(2):
            f0 = first[half][1]
            fill1(q, half, 2, near(f0, 1), 1, os)
            fill1(q, half, 3, near(f0, 3), 0, os)

    def phase1_rest(q, os):
        for half in range(2):
            f0 = first[half][1]
            hop1(q, half, 0, os).wait_recv()
            fill1(q, half, 4, near(f0, 1), 0, os, 0)
            hop1(q, half, 1, os).wait_recv()
            fill1(q, half, 5, near(f0, 3), 1, os, 1)

    def wait_rest1(q, half, os):
        n = 2 * q + half
        ref = rb1.at[n, pl.ds(2, 4), pl.ds(os[0] * eighth, len(os) * eighth)]
        send(ref, ref, rs_send.at[0], rs_recv.at[n, 2 + (3 if os == stay else 0)], **{X: 0}).wait_recv()

    def wait_rest2(q, half):
        n = 2 * q + half
        ref = rb2.at[n, pl.ds(2, 4)]
        send(ref, ref, rs_send.at[1], rs_recv.at[n, 8], **{X: 0}).wait_recv()

    def summed1(q, half, o, h, p):
        n = 2 * q + half
        return (
            own_block(q, half, first[half][1], o, h * eighth + p)
            + rb1[n, 3 - h, o * eighth + p].astype(F32)
            + rb1[n, 4 + h, o * eighth + p].astype(F32)
        )

    def over_part(body):
        lax.fori_loop(0, eighth, lambda p, _: (body(p), 0)[1], 0, unroll=8)

    def phase2(q):
        for half in range(2):
            n = 2 * q + half
            wait_rest1(q, half, onward)

            def far_block(p):
                sb2[n, 0, p] = summed1(q, half, 0, 0, p).astype(BF16)
                sb2[n, 1, p] = summed1(q, half, 0, 1, p).astype(BF16)

            over_part(far_block)
            hop2(q, half, 0).start()
            hop2(q, half, 1).start()
        for half in range(2):
            n = 2 * q + half

            def near_block(p):
                sb2[n, 2, p] = summed1(q, half, 1, 1, p).astype(BF16)
                sb2[n, 3, p] = summed1(q, half, 2, 0, p).astype(BF16)

            over_part(near_block)
            hop2(q, half, 2).start()
            hop2(q, half, 3).start()
        for half in range(2):
            n = 2 * q + half

            def kept(p):
                zside[n, 0, p] = summed1(q, half, 1, 0, p)
                zside[n, 1, p] = summed1(q, half, 2, 1, p)

            over_part(kept)

    def phase2_rest(q):
        for half in range(2):
            n = 2 * q + half
            hop2(q, half, 0).wait_recv()
            hop2(q, half, 1).wait_recv()

            def joined(p):
                sb2[n, 4, p] = (zside[n, 0, p] + rb2[n, 0, p].astype(F32)).astype(BF16)
                sb2[n, 5, p] = (zside[n, 1, p] + rb2[n, 1, p].astype(F32)).astype(BF16)

            over_part(joined)
            hop2(q, half, 4).start()
            hop2(q, half, 5).start()

    def place(q, half, m, value):
        for e in range(2):
            at = (pl.ds(q * group, group), lanes(half * part + m + e))
            w[at] = w[at] + value[e * group : (e + 1) * group]

    def stayed(q):
        for half in range(2):
            wait_rest1(q, half, stay)

            def body(p):
                place(q, half, 2 * p, summed1(q, half, 3, 0, p))
                place(q, half, quarter + 2 * p, summed1(q, half, 3, 1, p))

            over_part(body)

    def landed(q):
        for half in range(2):
            n = 2 * q + half
            wait_rest2(q, half)

            def body(p):
                place(q, half, 2 * p, rb2[n, 3, p].astype(F32) + rb2[n, 4, p].astype(F32))
                place(q, half, quarter + 2 * p, rb2[n, 2, p].astype(F32) + rb2[n, 5, p].astype(F32))

            over_part(body)

    phase1(0, onward)
    phase1(0, stay)
    crossed(1)
    products(1, 0, trips // 2)
    ring_start(2, ring_sum(1))
    products(1, trips // 2, trips)
    phase1_rest(0, onward)
    phase1(1, onward)
    phase1_rest(0, stay)
    whole[k0] = ring_sum(2) * F32(1.0 / total_rows)
    back = send(whole.at[k0], whole.at[k0], ea_send.at[2], ea_recv.at[4], **{K: 1 - k0})
    back.start()
    for q in range(2):
        ref = xg[q].at[pl.ds(0, 3 * seg_tiles)]
        send(ref, ref, ag_send.at[q, 0], ag_recv.at[q, 0], **{Y: up}).wait_send()
        ref = xg[q].at[pl.ds(0, 4 * seg_tiles)]
        send(ref, ref, ag_send.at[q, 1], ag_recv.at[q, 6], **{K: 1 - k0}).wait_send()
    back.wait_recv()
    products_of = jnp.concatenate([whole[0], whole[1]], axis=0)
    basis_gram = products_of[:width]
    guess = products_of[width:]
    exact = lax.Precision.HIGHEST

    def full(a, b, dims=(((1,), (0,)), ((), ()))):
        return lax.dot_general(a, b, dims, precision=exact, preferred_element_type=F32)

    guess_left = full(guess, basis_gram) - guess

    def paired(a):
        high, low = halves(a)
        top = jnp.concatenate([high, high], axis=1)
        return jnp.concatenate([top, jnp.concatenate([low, jnp.zeros_like(low)], axis=1)], axis=0)

    guess_pair = paired(guess)

    def lessen(i, _):
        at = pl.ds(pl.multiple_of(i * CHUNK, CHUNK), CHUNK)
        both = dot(guess_pair, q2[:, at])
        w[:, at] = w[:, at] - (both[:rhs] + both[rhs:])
        return 0

    lax.fori_loop(0, seg // CHUNK, lessen, 0)
    phase1_rest(1, onward)
    phase2(0)
    phase1(1, stay)

    def turn(i, _):
        at = pl.ds(pl.multiple_of(i * 128, 128), 128)
        flat = jnp.concatenate([basis[k, :, at] for k in range(blocks)], axis=0).T
        high, low = halves(flat)
        qt[at, pl.ds(0, width)] = high
        qt[at, pl.ds(width, width)] = low
        return 0

    lax.fori_loop(0, seg_tiles, turn, 0, unroll=4)
    phase2(1)
    phase2_rest(0)
    phase1_rest(1, stay)
    stayed(0)
    phase2_rest(1)
    landed(0)
    stayed(1)
    landed(1)

    def inner_copy(d):
        p = lax.rem(c0 + d, 8)
        ref = inner.at[c0]
        return send(ref, ref, ar_send.at[0], ar_recv.at[0], **{Y: p // 2, K: lax.rem(p, 2)})

    def outer_copy(d):
        p = lax.rem(r0 + d, 16)
        ref = outer.at[r0]
        return send(ref, ref, ar_send.at[1], ar_recv.at[1], **{X: p // 4, Z: lax.rem(p, 4)})

    def inner_all():
        ref = inner.at[pl.ds(0, 7)]
        return send(ref, ref, ar_send.at[0], ar_recv.at[0], **{Y: 0})

    def outer_all():
        ref = outer.at[pl.ds(0, 15)]
        return send(ref, ref, ar_send.at[1], ar_recv.at[1], **{X: 0})

    def project(i, acc):
        at = pl.ds(pl.multiple_of(i * LONG, LONG), LONG)
        stack = jnp.concatenate(halves(w[:, at]), axis=0)
        return acc[0] + dot(stack, qt[at, :]), acc[1] + dot(stack, stack, NT)

    with_basis, with_self = lax.fori_loop(
        0, seg // LONG, project, (jnp.zeros((2 * rhs, 2 * width), F32), jnp.zeros((2 * rhs, 2 * rhs), F32))
    )
    inner[c0, pl.ds(0, rhs)] = with_basis[:rhs, :width] + with_basis[rhs:, :width] + with_basis[:rhs, width:]
    with_self = with_self[:rhs, :rhs] + with_self[rhs:, :rhs] + with_self[:rhs, rhs:]
    folded = jnp.concatenate([with_self[:8], with_self[8:], jnp.zeros((8, 128 - 2 * rhs), F32)], axis=1)
    inner[c0, pl.ds(rhs, 8)] = folded
    for d in range(1, 8):
        inner_copy(d).start()
    inner_all().wait_recv()
    acc = inner[0]
    for i in range(1, 8):
        acc = acc + inner[i]
    outer[r0] = acc
    for d in range(1, 16):
        outer_copy(d).start()
    outer_all().wait_recv()
    acc = outer[0]
    for i in range(1, 16):
        acc = acc + outer[i]
    acc = acc * F32(1.0 / total_rows)
    reduced = acc[:rhs]
    rest = reduced + guess_left
    coef_ref[...] = (rest + guess).T
    basis_gram = jnp.concatenate([whole[0], whole[1]], axis=0)[:width]
    turned = full(rest, basis_gram) - reduced
    cross = full(turned, rest, NT) - full(rest, reduced, NT)
    gram = jnp.concatenate([acc[rhs:, :rhs], acc[rhs:, rhs : 2 * rhs]], axis=0) + cross
    gram = jnp.concatenate([gram, jnp.zeros((rhs, 128 - rhs), F32)], axis=1)

    row = lax.broadcasted_iota(jnp.int32, (rhs, 128), 0)
    lane = lax.broadcasted_iota(jnp.int32, (rhs, 128), 1)
    m = jnp.where(lane < rhs, gram, jnp.where(lane - rhs == row, F32(1), F32(0)))
    for k in range(rhs - 1):
        column = jnp.broadcast_to(m[:, k : k + 1], m.shape)
        m = m - jnp.where(row > k, column * (1.0 / column[k : k + 1, :]), F32(0)) * m[k : k + 1, :]
    pivots = jnp.sum(jnp.where(lane == row, m, F32(0)), axis=1, keepdims=True)
    m = m / jnp.sqrt(pivots)
    tri_ref[...] = jnp.where(lane >= row, m, F32(0))[:, :rhs]
    inverse = m[:, rhs : 2 * rhs]
    pairs_ref[:, pl.ds(0, 2 * width)] = paired(-full(inverse, rest))
    pairs_ref[:, pl.ds(2 * width, 128)] = jnp.concatenate(
        [paired(inverse), jnp.zeros((2 * rhs, 128 - 2 * rhs), BF16)], axis=1
    )
    send(sb1, sb1, rs_send.at[0], rs_recv.at[0, 0], **{X: 0}).wait_send()
    send(sb2, sb2, rs_send.at[1], rs_recv.at[0, 0], **{X: 0}).wait_send()
    inner_all().wait_send()
    outer_all().wait_send()
    to_pair.wait_send()
    back.wait_send()
    ref = ring.at[:, pl.ds(0, 3)]
    send(ref, ref, ea_send.at[1], ea_recv.at[1], **{X: 0}).wait_send()


def finish(w, q2, pairs, coef, tri, out_hbm, coef_hbm, tri_hbm, made, sem):
    rhs, seg = w.shape
    deep = q2.shape[0]
    count = seg // FINISH
    copies = [
        pltpu.make_async_copy(coef, coef_hbm, sem.at[count]),
        pltpu.make_async_copy(tri, tri_hbm, sem.at[count + 1]),
    ]
    for copy in copies:
        copy.start()
    for i in range(count):
        at = pl.ds(i * FINISH, FINISH)
        stack = jnp.concatenate(halves(w[:, at]), axis=0)
        both = dot(pairs[:, :deep], q2[:, at]) + dot(pairs[:, deep : deep + 2 * rhs], stack)
        made[:, at] = both[:rhs] + both[rhs:]
        copies.append(pltpu.make_async_copy(made.at[:, at], out_hbm.at[:, at], sem.at[i]))
        copies[-1].start()
    for copy in copies:
        copy.wait()


def local(basis_blocks, tile_values, tile_rows, tile_column, tile_count, diagonal):
    blocks, rhs, seg = basis_blocks.shape
    slots = tile_values.shape[2]
    seg_tiles = seg // 128
    part = seg_tiles // 2
    total_rows = seg * 128
    block_tiles = seg_tiles * 16

    vmem = pl.BlockSpec(memory_space=pltpu.VMEM)
    hbm = pl.BlockSpec(memory_space=pl.ANY)
    dma = pltpu.SemaphoreType.DMA
    tile = (rhs, 128)
    held = pl.pallas_call(
        functools.partial(kernel, total_rows),
        out_shape=(
            pltpu.VMEM((rhs, seg), F32),
            pltpu.VMEM((2 * blocks * rhs, seg), BF16),
            pltpu.VMEM((2 * rhs, 2 * blocks * rhs + 128), BF16),
            pltpu.VMEM((blocks * rhs, rhs), F32),
            pltpu.VMEM((rhs, rhs), F32),
        ),
        in_specs=[hbm] * 6,
        out_specs=(vmem,) * 5,
        scratch_shapes=[
            pltpu.VMEM((1, 1), jnp.int32),
            pltpu.SMEM((1, 1, slots), jnp.int32),
            pltpu.VMEM((1, slots), jnp.int32),
            pltpu.VMEM((1, seg), F32),
            pltpu.VMEM((blocks, rhs, seg), F32),
            pltpu.VMEM((slots, 128, 128), BF16),
            pltpu.VMEM((8 * seg_tiles, rhs // 2, 128), BF16),
            pltpu.VMEM((8 * seg_tiles, rhs // 2, 128), BF16),
            pltpu.VMEM((2, slots + 8, rhs // 2, 128), F32),
            pltpu.VMEM((seg, 2 * blocks * rhs), BF16),
            pltpu.VMEM((4, 6, part, *tile), BF16),
            pltpu.VMEM((4, 6, part, *tile), BF16),
            pltpu.VMEM((4, 6, part // 4, *tile), BF16),
            pltpu.VMEM((4, 6, part // 4, *tile), BF16),
            pltpu.VMEM((4, 2, part // 4, *tile), F32),
            pltpu.VMEM((1, slots), jnp.int32),
            pltpu.VMEM((1, block_tiles), jnp.int32),
            pltpu.SMEM((1, slots), jnp.int32),
            pltpu.SMEM((1, block_tiles), jnp.int32),
            pltpu.VMEM((9 * rhs, 128), F32),
            pltpu.VMEM((9 * rhs // 2, 128), F32),
            pltpu.VMEM((3, 4, 9 * rhs // 2, 128), F32),
            pltpu.VMEM((2, 9 * rhs // 2, 128), F32),
            pltpu.VMEM((8, rhs + 8, 128), F32),
            pltpu.VMEM((16, rhs + 8, 128), F32),
            dma((12,)),
            dma((2, 2)),
            dma((2, 7)),
            dma((2,)),
            dma((4, 9)),
            dma((3,)),
            dma((5,)),
            dma((2,)),
            dma((2,)),
        ],
        compiler_params=pltpu.CompilerParams(
            collective_id=0, has_side_effects=True, vmem_limit_bytes=50 * 1024 * 1024
        ),
        name="step",
    )(tile_count, tile_column, tile_rows[0], basis_blocks, tile_values[0, 0], diagonal[None, :])
    new_block, coef, triangle = pl.pallas_call(
        finish,
        out_shape=(
            jax.ShapeDtypeStruct((rhs, seg), F32),
            jax.ShapeDtypeStruct((blocks * rhs, rhs), F32),
            jax.ShapeDtypeStruct((rhs, rhs), F32),
        ),
        in_specs=[vmem] * 5,
        out_specs=(hbm,) * 3,
        scratch_shapes=[pltpu.VMEM((rhs, seg), F32), dma((seg // FINISH + 2,))],
        compiler_params=pltpu.CompilerParams(vmem_limit_bytes=4 * 1024 * 1024),
        name="finish",
    )(*[pltpu.with_memory_space_constraint(a, pltpu.VMEM) for a in held])
    return new_block, coef.reshape(blocks, rhs, rhs), triangle


def solution(mesh):
    split = Mesh(mesh.devices.reshape(4, 4, 4, 2), (X, Z, Y, K))
    placed = (
        P(None, None, COL_ROW),
        P(COL, ROW, None, None, None),
        P(COL, ROW, None),
        P(COL, ROW, None),
        P(COL, ROW),
        P(COL_ROW),
    )
    return jax.shard_map(
        local, mesh=split, in_specs=placed, out_specs=(P(None, COL_ROW), P(), P()), check_vma=False
    )
```

```python
import functools

import jax
import jax.numpy as jnp
from jax import lax
from jax.experimental import pallas as pl
from jax.experimental.pallas import tpu as pltpu
from jax.sharding import Mesh
from jax.sharding import PartitionSpec as P

X, Z, Y, K = "row_0", "row_1", "col_0", "col_1"
ROW = (X, Z)
COL = (Y, K)
COL_ROW = (Y, K, X, Z)
MESH = pl.DeviceIdType.MESH
F32, BF16 = jnp.float32, jnp.bfloat16
NT = (((1,), (1,)), ((), ()))
CHUNK = 1024
LONG = 4096
FINISH = 2048


def send(src, dst, send_sem, recv_sem, **to):
    return pltpu.make_async_remote_copy(
        src_ref=src, dst_ref=dst, send_sem=send_sem, recv_sem=recv_sem, device_id=to, device_id_type=MESH
    )


def halves(value):
    high = value.astype(BF16)
    return high, (value - high.astype(F32)).astype(BF16)


def dot(a, b, dims=(((1,), (0,)), ((), ()))):
    return lax.dot_general(a, b, dims, preferred_element_type=F32)


def lanes(m):
    return pl.ds(pl.multiple_of(m * 128, 128), 128)


def kernel(
    total_rows,
    count_hbm, cols_hbm, rows_hbm, basis_hbm, tiles_hbm, diag_hbm,
    w, q2, pairs_ref, coef_ref, tri_ref,
    count_ref, cols_ref, rows_ref, diag_ref,
    basis, tiles, xg0, xg1, chain, qt,
    sb1, rb1, sb2, rb2, zside,
    prev_vec, last_vec, prev_ref, last_ref,
    mine, pair, ring, whole, inner, outer,
    load_sem, ag_send, ag_recv, rs_send, rs_recv, ea_send, ea_recv, ar_send, ar_recv,
):
    x0, z0, y0, k0 = (lax.axis_index(a) for a in (X, Z, Y, K))
    blocks, rhs, seg = basis.shape
    slots = tiles.shape[0]
    seg_tiles = seg // 128
    part = seg_tiles // 2
    quarter = part // 2
    c0 = y0 * 2 + k0
    r0 = x0 * 4 + z0

    barrier = pltpu.get_barrier_semaphore()
    inner_peers = [lax.rem(c0 + d, 8) for d in range(1, 8)]
    outer_peers = [lax.rem(r0 + d, 16) for d in range(1, 16)]
    for p in inner_peers:
        pl.semaphore_signal(barrier, inc=1, device_id={Y: p // 2, K: lax.rem(p, 2)}, device_id_type=MESH)
    for p in outer_peers:
        pl.semaphore_signal(barrier, inc=1, device_id={X: p // 4, Z: lax.rem(p, 4)}, device_id_type=MESH)

    load_vector = pltpu.make_async_copy(basis_hbm.at[blocks - 1], basis.at[blocks - 1], load_sem.at[0])
    load_basis = pltpu.make_async_copy(
        basis_hbm.at[pl.ds(0, blocks - 1)], basis.at[pl.ds(0, blocks - 1)], load_sem.at[1]
    )
    load_vector.start()
    load_basis.start()
    piece = slots // 4
    loads = [
        pltpu.make_async_copy(
            tiles_hbm.at[pl.ds(i * piece, piece)], tiles.at[pl.ds(i * piece, piece)], load_sem.at[2 + i]
        )
        for i in range(4)
    ]
    small = [
        pltpu.make_async_copy(a, b, load_sem.at[8 + i])
        for i, (a, b) in enumerate(
            ((diag_hbm, diag_ref), (rows_hbm, rows_ref), (count_hbm, count_ref), (cols_hbm, cols_ref))
        )
    ]
    for copy in small + loads:
        copy.start()

    load_vector.wait()
    own = c0 * seg_tiles

    group = rhs // 2
    xg = (xg0, xg1)

    def to_tiles(q):
        def body(m, _):
            xg[q][own + m] = basis[blocks - 1, pl.ds(q * group, group), lanes(m)].astype(BF16)
            return 0

        lax.fori_loop(0, seg_tiles, body, 0, unroll=8)

    to_tiles(0)
    pl.semaphore_wait(barrier, 22)

    up, down, far = lax.rem(y0 + 1, 4), lax.rem(y0 + 3, 4), lax.rem(y0 + 2, 4)

    def chunk(q, y, k, h):
        return xg[q].at[pl.ds((y * 2 + k) * seg_tiles + h * part, part)]

    def hop(q, i, y, h, to):
        ref = chunk(q, y, k0, h)
        return send(ref, ref, ag_send.at[q, 0], ag_recv.at[q, i], **{Y: to})

    def across(q, y, h, k):
        ref = chunk(q, y, k, h)
        return send(ref, ref, ag_send.at[q, 1], ag_recv.at[q, 6], **{K: 1 - k0})

    hops = [
        [hop(q, 0, y0, 0, up), hop(q, 1, y0, 1, up), hop(q, 2, y0, 1, down), hop(q, 3, y0, 0, down)]
        for q in range(2)
    ]
    arrive = [
        [
            hop(q, 0, down, 0, up), hop(q, 1, down, 1, up), hop(q, 2, up, 1, down),
            hop(q, 3, up, 0, down), hop(q, 4, far, 0, up), hop(q, 5, far, 1, down),
        ]
        for q in range(2)
    ]
    forward = [[hop(q, 4, down, 0, up), hop(q, 5, up, 1, down)] for q in range(2)]
    places = list(enumerate((y0, down, up, far)))
    over = [[across(q, y, h, k0) for i, y in places for h in range(2)] for q in range(2)]

    def crossed(q):
        ref = xg[q].at[pl.ds(0, 4 * seg_tiles)]
        send(ref, ref, ag_send.at[q, 1], ag_recv.at[q, 6], **{K: 1 - k0}).wait_recv()

    def depart(q):
        for i in (0, 2, 1, 3):
            hops[q][i].start()
        over[q][0].start()
        over[q][1].start()

    def pass_on(q):
        for i, j, f in ((0, 2, 0), (2, 5, 1)):
            arrive[q][i].wait_recv()
            forward[q][f].start()
            over[q][j].start()

    def take(q, pairs):
        for i, j in pairs:
            arrive[q][i].wait_recv()
            over[q][j].start()

    depart(0)
    to_tiles(1)

    load_basis.wait()
    for copy in small:
        copy.wait()

    width = blocks * rhs

    def split_basis(i, acc):
        at = pl.ds(pl.multiple_of(i * CHUNK, CHUNK), CHUNK)
        for k in range(blocks):
            high, low = halves(basis[k, :, at])
            q2[pl.ds(k * rhs, rhs), at] = high
            q2[pl.ds(width + k * rhs, rhs), at] = low
        shifted = basis[blocks - 1, :, at] * diag_ref[:, at]
        w[:, at] = shifted
        stack = jnp.concatenate([q2[:, at], shifted.astype(BF16)], axis=0)
        return acc + dot(stack, q2[pl.ds(0, width), at], NT)

    made = lax.fori_loop(0, seg // CHUNK, split_basis, jnp.zeros((2 * width + rhs, width), F32))
    mine[pl.ds(0, width)] = made[:width] + made[width : 2 * width] + made[width : 2 * width].T
    mine[pl.ds(width, rhs)] = made[2 * width :]

    load = (width + rhs) // 2
    ring_axes = ((X, x0), (Z, z0), (Y, y0))
    to_pair = send(
        mine.at[pl.ds(pl.multiple_of((1 - k0) * load, 8), load)], pair, ea_send.at[0], ea_recv.at[0], **{K: 1 - k0}
    )
    to_pair.start()

    def ring_copy(i, d):
        axis, pos = ring_axes[i]
        ref = ring.at[i, pos]
        return send(ref, ref, ea_send.at[1], ea_recv.at[1 + i], **{axis: lax.rem(pos + d, 4)})

    def ring_start(i, value):
        ring[i, ring_axes[i][1]] = value
        for d in range(1, 4):
            ring_copy(i, d).start()

    def ring_sum(i):
        ref = ring.at[i, pl.ds(0, 3)]
        send(ref, ref, ea_send.at[1], ea_recv.at[1 + i], **{ring_axes[i][0]: 0}).wait_recv()
        return (ring[i, 0] + ring[i, 1]) + (ring[i, 2] + ring[i, 3])

    lane_slot = lax.broadcasted_iota(jnp.int32, (1, 128), 1)
    sub_slot = lax.broadcasted_iota(jnp.int32, (128, 128), 0)
    count = count_ref[...]
    row_lanes, row_subs = [], []
    for c in range(slots // 128):
        row_c = rows_ref[:, pl.ds(c * 128, 128)]
        row_c = jnp.where(lane_slot + c * 128 < count, row_c, -1)
        row_lanes.append(row_c)
        row_subs.append(jnp.broadcast_to(row_c, (128, 128)).T)
    for c in range(slots // 128):
        best = jnp.zeros((1, 128), jnp.int32)
        for e in range(c + 1):
            found = row_subs[e] == row_lanes[c]
            if e == c:
                found = found & (sub_slot < lane_slot)
            best = jnp.maximum(best, jnp.max(jnp.where(found, sub_slot + (e * 128 + 1), 0), axis=0, keepdims=True))
        prev_vec[:, pl.ds(c * 128, 128)] = best
    for c in range(last_vec.shape[1] // 128):
        best = jnp.zeros((1, 128), jnp.int32)
        for e in range(slots // 128):
            found = row_subs[e] == lane_slot + c * 128
            best = jnp.maximum(best, jnp.max(jnp.where(found, sub_slot + (e * 128 + 1), 0), axis=0, keepdims=True))
        last_vec[:, pl.ds(c * 128, 128)] = best
    tables = [
        pltpu.make_async_copy(prev_vec, prev_ref, load_sem.at[6]),
        pltpu.make_async_copy(last_vec, last_ref, load_sem.at[7]),
    ]
    for copy in tables:
        copy.start()

    pass_on(0)
    depart(1)
    to_pair.wait_recv()
    ring_start(0, mine[pl.ds(pl.multiple_of(k0 * load, 8), load)] + pair[...])
    take(0, ((1, 3), (3, 4), (4, 6), (5, 7)))
    crossed(0)
    for copy in loads + tables:
        copy.wait()

    step = 96
    trips = slots // step

    def products(q, start, stop):

        def body(i, _):
            base = i * step
            made = [
                dot(xg[q][jnp.clip(cols_ref[0, 0, base + j], 0, 8 * seg_tiles - 1)], tiles[base + j])
                for j in range(step)
            ]
            for j in range(step):
                chain[q, base + j + 1] = made[j] + chain[q, prev_ref[0, base + j]]
            return 0

        lax.fori_loop(start, stop, body, 0)

    chain[0, 0] = jnp.zeros((group, 128), F32)
    chain[1, 0] = jnp.zeros((group, 128), F32)
    products(0, 0, trips // 4)
    pass_on(1)
    take(1, ((1, 3), (3, 4)))
    products(0, trips // 4, trips // 2)
    ring_start(1, ring_sum(0))
    products(0, trips // 2, trips)
    take(1, ((4, 6), (5, 7)))

    first = ((X, x0), (Z, z0))
    second = ((Z, z0), (X, x0))

    def near(pos, d):
        return lax.rem(pos + d, 4)

    def partial(q, half, f, g, p):
        r = f * 4 + g if half == 0 else g * 4 + f
        at = r * seg_tiles + half * part + 2 * p
        return jnp.concatenate([chain[q, last_ref[0, at]], chain[q, last_ref[0, at + 1]]], axis=0)

    ahead = (2, 1, 3, 0)
    eighth = quarter // 2
    onward, stay = (0, 1, 2), (3,)

    def hop1(q, half, i, os):
        axis, pos = first[half]
        n = 2 * q + half
        at = pl.ds(os[0] * eighth, len(os) * eighth)
        return send(
            sb1.at[n, i, at], rb1.at[n, i, at], rs_send.at[0], rs_recv.at[n, min(i, 2) + (3 if os == stay else 0)],
            **{axis: near(pos, 1 if i % 2 == 0 else 3)},
        )

    def hop2(q, half, i):
        axis, pos = second[half]
        n = 2 * q + half
        return send(
            sb2.at[n, i], rb2.at[n, i], rs_send.at[1], rs_recv.at[n, 6 + min(i, 2)],
            **{axis: near(pos, 1 if i % 2 == 0 else 3)},
        )

    def own_block(q, half, f, o, p):
        return partial(q, half, f, near(second[half][1], ahead[o]), p)

    def fill1(q, half, i, f, h, os, arrived=None):
        n = 2 * q + half

        def body(p, _):
            for o in os:
                value = own_block(q, half, f, o, h * eighth + p)
                if arrived is not None:
                    value = value + rb1[n, arrived, o * eighth + p].astype(F32)
                sb1[n, i, o * eighth + p] = value.astype(BF16)
            return 0

        lax.fori_loop(0, eighth, body, 0, unroll=8)
        hop1(q, half, i, os).start()

    def phase1(q, os):
        for half in range(2):
            f0 = first[half][1]
            fill1(q, half, 0, near(f0, 2), 0, os)
            fill1(q, half, 1, near(f0, 2), 1, os)
        for half in range(2):
            f0 = first[half][1]
            fill1(q, half, 2, near(f0, 1), 1, os)
            fill1(q, half, 3, near(f0, 3), 0, os)

    def phase1_rest(q, os):
        for half in range(2):
            f0 = first[half][1]
            hop1(q, half, 0, os).wait_recv()
            fill1(q, half, 4, near(f0, 1), 0, os, 0)
            hop1(q, half, 1, os).wait_recv()
            fill1(q, half, 5, near(f0, 3), 1, os, 1)

    def wait_rest1(q, half, os):
        n = 2 * q + half
        ref = rb1.at[n, pl.ds(2, 4), pl.ds(os[0] * eighth, len(os) * eighth)]
        send(ref, ref, rs_send.at[0], rs_recv.at[n, 2 + (3 if os == stay else 0)], **{X: 0}).wait_recv()

    def wait_rest2(q, half):
        n = 2 * q + half
        ref = rb2.at[n, pl.ds(2, 4)]
        send(ref, ref, rs_send.at[1], rs_recv.at[n, 8], **{X: 0}).wait_recv()

    def summed1(q, half, o, h, p):
        n = 2 * q + half
        return (
            own_block(q, half, first[half][1], o, h * eighth + p)
            + rb1[n, 3 - h, o * eighth + p].astype(F32)
            + rb1[n, 4 + h, o * eighth + p].astype(F32)
        )

    def over_part(body):
        lax.fori_loop(0, eighth, lambda p, _: (body(p), 0)[1], 0, unroll=8)

    def phase2(q):
        for half in range(2):
            n = 2 * q + half
            wait_rest1(q, half, onward)

            def far_block(p):
                sb2[n, 0, p] = summed1(q, half, 0, 0, p).astype(BF16)
                sb2[n, 1, p] = summed1(q, half, 0, 1, p).astype(BF16)

            over_part(far_block)
            hop2(q, half, 0).start()
            hop2(q, half, 1).start()
        for half in range(2):
            n = 2 * q + half

            def near_block(p):
                sb2[n, 2, p] = summed1(q, half, 1, 1, p).astype(BF16)
                sb2[n, 3, p] = summed1(q, half, 2, 0, p).astype(BF16)

            over_part(near_block)
            hop2(q, half, 2).start()
            hop2(q, half, 3).start()
        for half in range(2):
            n = 2 * q + half

            def kept(p):
                zside[n, 0, p] = summed1(q, half, 1, 0, p)
                zside[n, 1, p] = summed1(q, half, 2, 1, p)

            over_part(kept)

    def phase2_rest(q):
        for half in range(2):
            n = 2 * q + half
            hop2(q, half, 0).wait_recv()
            hop2(q, half, 1).wait_recv()

            def joined(p):
                sb2[n, 4, p] = (zside[n, 0, p] + rb2[n, 0, p].astype(F32)).astype(BF16)
                sb2[n, 5, p] = (zside[n, 1, p] + rb2[n, 1, p].astype(F32)).astype(BF16)

            over_part(joined)
            hop2(q, half, 4).start()
            hop2(q, half, 5).start()

    def place(q, half, m, value):
        for e in range(2):
            at = (pl.ds(q * group, group), lanes(half * part + m + e))
            w[at] = w[at] + value[e * group : (e + 1) * group]

    def stayed(q):
        for half in range(2):
            wait_rest1(q, half, stay)

            def body(p):
                place(q, half, 2 * p, summed1(q, half, 3, 0, p))
                place(q, half, quarter + 2 * p, summed1(q, half, 3, 1, p))

            over_part(body)

    def landed(q):
        for half in range(2):
            n = 2 * q + half
            wait_rest2(q, half)

            def body(p):
                place(q, half, 2 * p, rb2[n, 3, p].astype(F32) + rb2[n, 4, p].astype(F32))
                place(q, half, quarter + 2 * p, rb2[n, 2, p].astype(F32) + rb2[n, 5, p].astype(F32))

            over_part(body)

    phase1(0, onward)
    phase1(0, stay)
    crossed(1)
    products(1, 0, trips // 2)
    ring_start(2, ring_sum(1))
    products(1, trips // 2, trips)
    phase1_rest(0, onward)
    phase1(1, onward)
    phase1_rest(0, stay)
    whole[k0] = ring_sum(2) * F32(1.0 / total_rows)
    back = send(whole.at[k0], whole.at[k0], ea_send.at[2], ea_recv.at[4], **{K: 1 - k0})
    back.start()
    for q in range(2):
        ref = xg[q].at[pl.ds(0, 3 * seg_tiles)]
        send(ref, ref, ag_send.at[q, 0], ag_recv.at[q, 0], **{Y: up}).wait_send()
        ref = xg[q].at[pl.ds(0, 4 * seg_tiles)]
        send(ref, ref, ag_send.at[q, 1], ag_recv.at[q, 6], **{K: 1 - k0}).wait_send()
    back.wait_recv()
    products_of = jnp.concatenate([whole[0], whole[1]], axis=0)
    basis_gram = products_of[:width]
    guess = products_of[width:]
    exact = lax.Precision.HIGHEST

    def full(a, b, dims=(((1,), (0,)), ((), ()))):
        return lax.dot_general(a, b, dims, precision=exact, preferred_element_type=F32)

    guess_left = full(guess, basis_gram) - guess

    def paired(a):
        high, low = halves(a)
        top = jnp.concatenate([high, high], axis=1)
        return jnp.concatenate([top, jnp.concatenate([low, jnp.zeros_like(low)], axis=1)], axis=0)

    guess_pair = paired(guess)

    def lessen(i, _):
        at = pl.ds(pl.multiple_of(i * CHUNK, CHUNK), CHUNK)
        both = dot(guess_pair, q2[:, at])
        w[:, at] = w[:, at] - (both[:rhs] + both[rhs:])
        return 0

    lax.fori_loop(0, seg // CHUNK, lessen, 0)
    phase1_rest(1, onward)
    phase2(0)
    phase1(1, stay)

    def turn(i, _):
        at = pl.ds(pl.multiple_of(i * 128, 128), 128)
        flat = jnp.concatenate([basis[k, :, at] for k in range(blocks)], axis=0).T
        high, low = halves(flat)
        qt[at, pl.ds(0, width)] = high
        qt[at, pl.ds(width, width)] = low
        return 0

    lax.fori_loop(0, seg_tiles, turn, 0, unroll=4)
    phase2(1)
    phase2_rest(0)
    phase1_rest(1, stay)
    stayed(0)
    phase2_rest(1)
    landed(0)
    stayed(1)
    landed(1)

    def inner_copy(d):
        p = lax.rem(c0 + d, 8)
        ref = inner.at[c0]
        return send(ref, ref, ar_send.at[0], ar_recv.at[0], **{Y: p // 2, K: lax.rem(p, 2)})

    def outer_copy(d):
        p = lax.rem(r0 + d, 16)
        ref = outer.at[r0]
        return send(ref, ref, ar_send.at[1], ar_recv.at[1], **{X: p // 4, Z: lax.rem(p, 4)})

    def inner_all():
        ref = inner.at[pl.ds(0, 7)]
        return send(ref, ref, ar_send.at[0], ar_recv.at[0], **{Y: 0})

    def outer_all():
        ref = outer.at[pl.ds(0, 15)]
        return send(ref, ref, ar_send.at[1], ar_recv.at[1], **{X: 0})

    def project(i, acc):
        at = pl.ds(pl.multiple_of(i * LONG, LONG), LONG)
        stack = jnp.concatenate(halves(w[:, at]), axis=0)
        return acc[0] + dot(stack, qt[at, :]), acc[1] + dot(stack, stack, NT)

    with_basis, with_self = lax.fori_loop(
        0, seg // LONG, project, (jnp.zeros((2 * rhs, 2 * width), F32), jnp.zeros((2 * rhs, 2 * rhs), F32))
    )
    inner[c0, pl.ds(0, rhs)] = with_basis[:rhs, :width] + with_basis[rhs:, :width] + with_basis[:rhs, width:]
    with_self = with_self[:rhs, :rhs] + with_self[rhs:, :rhs] + with_self[:rhs, rhs:]
    folded = jnp.concatenate([with_self[:8], with_self[8:], jnp.zeros((8, 128 - 2 * rhs), F32)], axis=1)
    inner[c0, pl.ds(rhs, 8)] = folded
    for d in range(1, 8):
        inner_copy(d).start()
    inner_all().wait_recv()
    acc = inner[0]
    for i in range(1, 8):
        acc = acc + inner[i]
    outer[r0] = acc
    for d in range(1, 16):
        outer_copy(d).start()
    outer_all().wait_recv()
    acc = outer[0]
    for i in range(1, 16):
        acc = acc + outer[i]
    acc = acc * F32(1.0 / total_rows)
    reduced = acc[:rhs]
    rest = reduced + guess_left
    coef_ref[...] = (rest + guess).T
    basis_gram = jnp.concatenate([whole[0], whole[1]], axis=0)[:width]
    turned = full(rest, basis_gram) - reduced
    cross = full(turned, rest, NT) - full(rest, reduced, NT)
    gram = jnp.concatenate([acc[rhs:, :rhs], acc[rhs:, rhs : 2 * rhs]], axis=0) + cross
    gram = jnp.concatenate([gram, jnp.zeros((rhs, 128 - rhs), F32)], axis=1)

    row = lax.broadcasted_iota(jnp.int32, (rhs, 128), 0)
    lane = lax.broadcasted_iota(jnp.int32, (rhs, 128), 1)
    m = jnp.where(lane < rhs, gram, jnp.where(lane - rhs == row, F32(1), F32(0)))
    for k in range(rhs - 1):
        column = jnp.broadcast_to(m[:, k : k + 1], m.shape)
        m = m - jnp.where(row > k, column * (1.0 / column[k : k + 1, :]), F32(0)) * m[k : k + 1, :]
    pivots = jnp.sum(jnp.where(lane == row, m, F32(0)), axis=1, keepdims=True)
    m = m / jnp.sqrt(pivots)
    tri_ref[...] = jnp.where(lane >= row, m, F32(0))[:, :rhs]
    inverse = m[:, rhs : 2 * rhs]
    pairs_ref[:, pl.ds(0, 2 * width)] = paired(-full(inverse, rest))
    pairs_ref[:, pl.ds(2 * width, 128)] = jnp.concatenate(
        [paired(inverse), jnp.zeros((2 * rhs, 128 - 2 * rhs), BF16)], axis=1
    )
    send(sb1, sb1, rs_send.at[0], rs_recv.at[0, 0], **{X: 0}).wait_send()
    send(sb2, sb2, rs_send.at[1], rs_recv.at[0, 0], **{X: 0}).wait_send()
    inner_all().wait_send()
    outer_all().wait_send()
    to_pair.wait_send()
    back.wait_send()
    ref = ring.at[:, pl.ds(0, 3)]
    send(ref, ref, ea_send.at[1], ea_recv.at[1], **{X: 0}).wait_send()


def finish(w, q2, pairs, coef, tri, out_hbm, coef_hbm, tri_hbm, made, sem):
    rhs, seg = w.shape
    deep = q2.shape[0]
    count = seg // FINISH
    copies = [
        pltpu.make_async_copy(coef, coef_hbm, sem.at[count]),
        pltpu.make_async_copy(tri, tri_hbm, sem.at[count + 1]),
    ]
    for copy in copies:
        copy.start()
    for i in range(count):
        at = pl.ds(i * FINISH, FINISH)
        stack = jnp.concatenate(halves(w[:, at]), axis=0)
        both = dot(pairs[:, :deep], q2[:, at]) + dot(pairs[:, deep : deep + 2 * rhs], stack)
        made[:, at] = both[:rhs] + both[rhs:]
        copies.append(pltpu.make_async_copy(made.at[:, at], out_hbm.at[:, at], sem.at[i]))
        copies[-1].start()
    for copy in copies:
        copy.wait()


def local(basis_blocks, tile_values, tile_rows, tile_column, tile_count, diagonal):
    blocks, rhs, seg = basis_blocks.shape
    slots = tile_values.shape[2]
    seg_tiles = seg // 128
    part = seg_tiles // 2
    total_rows = seg * 128
    block_tiles = seg_tiles * 16

    vmem = pl.BlockSpec(memory_space=pltpu.VMEM)
    hbm = pl.BlockSpec(memory_space=pl.ANY)
    dma = pltpu.SemaphoreType.DMA
    tile = (rhs, 128)
    held = pl.pallas_call(
        functools.partial(kernel, total_rows),
        out_shape=(
            pltpu.VMEM((rhs, seg), F32),
            pltpu.VMEM((2 * blocks * rhs, seg), BF16),
            pltpu.VMEM((2 * rhs, 2 * blocks * rhs + 128), BF16),
            pltpu.VMEM((blocks * rhs, rhs), F32),
            pltpu.VMEM((rhs, rhs), F32),
        ),
        in_specs=[hbm] * 6,
        out_specs=(vmem,) * 5,
        scratch_shapes=[
            pltpu.VMEM((1, 1), jnp.int32),
            pltpu.SMEM((1, 1, slots), jnp.int32),
            pltpu.VMEM((1, slots), jnp.int32),
            pltpu.VMEM((1, seg), F32),
            pltpu.VMEM((blocks, rhs, seg), F32),
            pltpu.VMEM((slots, 128, 128), BF16),
            pltpu.VMEM((8 * seg_tiles, rhs // 2, 128), BF16),
            pltpu.VMEM((8 * seg_tiles, rhs // 2, 128), BF16),
            pltpu.VMEM((2, slots + 8, rhs // 2, 128), F32),
            pltpu.VMEM((seg, 2 * blocks * rhs), BF16),
            pltpu.VMEM((4, 6, part, *tile), BF16),
            pltpu.VMEM((4, 6, part, *tile), BF16),
            pltpu.VMEM((4, 6, part // 4, *tile), BF16),
            pltpu.VMEM((4, 6, part // 4, *tile), BF16),
            pltpu.VMEM((4, 2, part // 4, *tile), F32),
            pltpu.VMEM((1, slots), jnp.int32),
            pltpu.VMEM((1, block_tiles), jnp.int32),
            pltpu.SMEM((1, slots), jnp.int32),
            pltpu.SMEM((1, block_tiles), jnp.int32),
            pltpu.VMEM((9 * rhs, 128), F32),
            pltpu.VMEM((9 * rhs // 2, 128), F32),
            pltpu.VMEM((3, 4, 9 * rhs // 2, 128), F32),
            pltpu.VMEM((2, 9 * rhs // 2, 128), F32),
            pltpu.VMEM((8, rhs + 8, 128), F32),
            pltpu.VMEM((16, rhs + 8, 128), F32),
            dma((12,)),
            dma((2, 2)),
            dma((2, 7)),
            dma((2,)),
            dma((4, 9)),
            dma((3,)),
            dma((5,)),
            dma((2,)),
            dma((2,)),
        ],
        compiler_params=pltpu.CompilerParams(
            collective_id=0, has_side_effects=True, vmem_limit_bytes=50 * 1024 * 1024
        ),
        name="step",
    )(tile_count, tile_column, tile_rows[0], basis_blocks, tile_values[0, 0], diagonal[None, :])
    new_block, coef, triangle = pl.pallas_call(
        finish,
        out_shape=(
            jax.ShapeDtypeStruct((rhs, seg), F32),
            jax.ShapeDtypeStruct((blocks * rhs, rhs), F32),
            jax.ShapeDtypeStruct((rhs, rhs), F32),
        ),
        in_specs=[vmem] * 5,
        out_specs=(hbm,) * 3,
        scratch_shapes=[pltpu.VMEM((rhs, seg), F32), dma((seg // FINISH + 2,))],
        compiler_params=pltpu.CompilerParams(vmem_limit_bytes=4 * 1024 * 1024),
        name="finish",
    )(*[pltpu.with_memory_space_constraint(a, pltpu.VMEM) for a in held])
    return new_block, coef.reshape(blocks, rhs, rhs), triangle


def solution(mesh):
    split = Mesh(mesh.devices.reshape(4, 4, 4, 2), (X, Z, Y, K))
    placed = (
        P(None, None, COL_ROW),
        P(COL, ROW, None, None, None),
        P(COL, ROW, None),
        P(COL, ROW, None),
        P(COL, ROW),
        P(COL_ROW),
    )
    return jax.shard_map(
        local, mesh=split, in_specs=placed, out_specs=(P(None, COL_ROW), P(), P()), check_vma=False
    )
```
